32 devices in a mesh: data: 2 (over x), c: 4 (over z), r: 4 (over y, core).
Axes of the slice: x: 2, y: 2, z: 4, core: 2. Of those that a mesh axis runs over, the one named last changes fastest.
Arguments:
- x: bfloat16 [4096, 3584], P(('data', 'r'), 'c'), parts along dimension 0
- w: bfloat16 [3584, 28672], P('r', 'c')
- dy: bfloat16 [4096, 28672], P(('data', 'r'), 'c'), parts along dimension 0
Outputs:
- output 1: bfloat16 [4096, 3584], P(('data', 'r'), 'c'), parts along dimension 0
- output 2: float32 [7168, 28672], P(('data', 'r'), 'c'), parts along dimension 0
There are 2 independent parts. The reference program is written for one: setup_inputs(seed, part) draws one part's arguments, and reference() takes and returns one part's arrays. A program takes and returns all parts, laid end to end along the dimension named above; an argument that names none is the same for every part.
All inputs are finite; a program needn't handle non-finite values.
Results may differ from the reference program's by a relative error of at most 0.001.
Values are sent between devices in bfloat16 or wider.
A program may use at most 1 GiB of HBM per device.

```python
import jax
import jax.numpy as jnp

T = 2048
K = 3584
N = 28672


def setup_inputs(seed: int = 0, part: int = 0) -> dict:
    key = jax.random.PRNGKey(seed)
    kw, kparts = jax.random.split(key)
    kx, kdy = jax.random.split(jax.random.fold_in(kparts, part))
    x = jax.random.normal(kx, (T, K), jnp.float32) * (N / (K * T)) ** 0.5
    w = jax.random.normal(kw, (K, N), jnp.float32) * K ** -0.5
    dy = jax.random.normal(kdy, (T, N), jnp.float32) * (K / N) ** 0.5
    return {"x": x.astype(jnp.bfloat16), "w": w.astype(jnp.bfloat16), "dy": dy.astype(jnp.bfloat16)}


def reference(x, w, dy):
    dx = jnp.dot(dy, w.T, preferred_element_type=jnp.float32).astype(jnp.bfloat16)
    dw = jnp.dot(x.T, dy, preferred_element_type=jnp.float32)
    return dx, dw
```

```python
import jax
import jax.numpy as jnp
from jax import lax
from jax.sharding import PartitionSpec as P


def solution(mesh):
    rows = P(("data", "r"), "c")
    n = mesh.shape["r"]
    swap = [(c * n + r, r * n + c) for c in range(n) for r in range(n)]

    def local(x, w, dy):
        dy_full = lax.all_gather(dy, "r", axis=0, tiled=True)
        x_swap = lax.ppermute(x, ("c", "r"), swap)
        x_full = lax.all_gather(x_swap, "c", axis=0, tiled=True)
        pdx = lax.dot_general(dy_full, w, (((1,), (1,)), ((), ())), preferred_element_type=jnp.float32)
        dx = lax.psum_scatter(pdx, "c", scatter_dimension=0, tiled=True).astype(jnp.bfloat16)
        dx = lax.ppermute(dx, ("c", "r"), swap)
        dw = lax.dot_general(x_full, dy_full, (((0,), (0,)), ((), ())), preferred_element_type=jnp.float32)
        return dx, dw

    return jax.shard_map(local, mesh=mesh, in_specs=(rows, P("r", "c"), rows), out_specs=(rows, rows), check_vma=False)
```

```python
import jax
import jax.numpy as jnp
from jax import lax
from jax.experimental import pallas as pl
from jax.experimental.pallas import tpu as pltpu
from jax.sharding import PartitionSpec as P

MESH = pl.DeviceIdType.MESH
PIECES = 4
STEPS = 2 * PIECES
SLOTS = 4


def pick(size, want):
    return want if size % want == 0 else 128


def kernel(
    x_ref, w_ref, dy_ref, dx_ref, dw_ref,
    dyf, wv, xf, pbuf, rb1, rb2, fbuf, obuf,
    ld_sem, w_sem, y_send, y_recv, d_send, d_recv, e_send, e_recv,
    z1_send, z1_recv, z2_send, z2_recv, f_send, f_recv,
    x_src, x_recv, x_left, x_right, o_sem,
):
    z, r = lax.axis_index("c"), lax.axis_index("r")
    y, k = r // 2, r % 2
    mate, over, over_mate = 2 * y + 1 - k, 2 * (1 - y) + k, 2 * (1 - y) + 1 - k
    zb, zh = z % 2, z // 2
    z1, z2 = 2 * zh + 1 - zb, 2 * (1 - zh) + zb
    tb, kb = x_ref.shape
    nb = dy_ref.shape[1]
    pr = tb // PIECES
    sub = pr // 2
    kc, nc = pick(nb, 1024), pick(nb, 512)

    def rows(block, p):
        return pl.ds(pl.multiple_of(block * tb + p * pr, pr), pr)

    def send(src, dst, ssem, rsem, c=None, rr=None):
        dev = {}
        if c is not None:
            dev["c"] = c
        if rr is not None:
            dev["r"] = rr
        return pltpu.make_async_remote_copy(
            src_ref=src, dst_ref=dst, send_sem=ssem, recv_sem=rsem, device_id=dev, device_id_type=MESH
        )

    def load(p):
        return pltpu.make_async_copy(dy_ref.at[pl.ds(p * pr, pr)], dyf.at[rows(r, p)], ld_sem.at[p])

    w_load = pltpu.make_async_copy(w_ref, wv, w_sem)
    for p in range(PIECES):
        load(p).start()
    w_load.start()

    barrier = pltpu.get_barrier_semaphore()
    for i in range(1, 16):
        peer = {"c": (z + i // 4) % 4, "r": (r + i % 4) % 4}
        pl.semaphore_signal(barrier, inc=1, device_id=peer, device_id_type=MESH)
    pl.semaphore_wait(barrier, 15)

    def xrows(t):
        return pl.ds(pl.multiple_of(t * tb, tb), tb)

    x_own = pltpu.make_async_copy(x_ref, xf.at[xrows(r)], x_recv.at[r])
    x_out = send(x_ref, xf.at[xrows(r)], x_src.at[0], x_recv.at[r], c=z, rr=z)

    @pl.when(r == z)
    def _():
        x_own.start()

    @pl.when(r != z)
    def _():
        x_out.start()

    def y_copy(p):
        return send(dyf.at[rows(r, p)], dyf.at[rows(r, p)], y_send.at[p], y_recv.at[p], rr=over)

    def d_copy(p):
        return send(dyf.at[rows(r, p)], dyf.at[rows(r, p)], d_send.at[p], d_recv.at[p], rr=mate)

    def e_copy(p):
        return send(dyf.at[rows(over, p)], dyf.at[rows(over, p)], e_send.at[p], e_recv.at[p], rr=mate)

    def y_arrival(p):
        return send(dyf.at[rows(over, p)], dyf.at[rows(over, p)], y_send.at[p], y_recv.at[p], rr=over)

    def d_arrival(p):
        return send(dyf.at[rows(mate, p)], dyf.at[rows(mate, p)], d_send.at[p], d_recv.at[p], rr=mate)

    def e_arrival(p):
        return send(dyf.at[rows(over_mate, p)], dyf.at[rows(over_mate, p)], e_send.at[p], e_recv.at[p], rr=mate)

    for p in range(PIECES):
        load(p).wait()
        y_copy(p).start()
        d_copy(p).start()

    dist = jnp.where(z >= r, z - r, r - z)

    def x_right_copy(t):
        return send(xf.at[xrows(t)], xf.at[xrows(t)], x_right.at[t], x_recv.at[t], c=z + 1)

    def x_left_copy(t):
        return send(xf.at[xrows(t)], xf.at[xrows(t)], x_left.at[t], x_recv.at[t], c=z - 1)

    go_right = jnp.logical_and(z >= r, z < 3)
    go_left = jnp.logical_and(z <= r, z > 0)

    def x_point(j):
        t = j - dist
        live = jnp.logical_and(t >= 0, t < 4)

        @pl.when(live)
        def _():
            pltpu.make_async_copy(x_ref, xf.at[xrows(t)], x_recv.at[t]).wait()

        @pl.when(jnp.logical_and(live, go_right))
        def _():
            x_right_copy(t).start()

        @pl.when(jnp.logical_and(live, go_left))
        def _():
            x_left_copy(t).start()

    def blocks(s):
        return (r, mate, s) if s < PIECES else (over, over_mate, s - PIECES)

    def z1_copy(s):
        half = pl.ds(pl.multiple_of((1 - zb) * pr, pr), pr)
        return send(pbuf.at[s % SLOTS, half], rb1.at[s], z1_send.at[s], z1_recv.at[s], c=z1)

    def kept(i):
        return pl.ds(pl.multiple_of(zb * pr + i * sub, sub), sub)

    def part(i):
        return pl.ds(pl.multiple_of(i * sub, sub), sub)

    def z2_copy(s):
        return send(pbuf.at[s % SLOTS, kept(1 - zh)], rb2.at[s], z2_send.at[s], z2_recv.at[s], c=z2)

    def f_start(s, begin):
        a, b, p = blocks(s)
        owner = a + zb * (b - a)
        dst = dx_ref.at[pl.ds(pl.multiple_of(p * pr + zh * sub, sub), sub)]
        away = jnp.logical_or(z != r, owner != r)

        @pl.when(away)
        def _():
            copy = send(fbuf.at[s], dst, f_send.at[s], f_recv.at[0], c=r, rr=owner)
            copy.start() if begin else copy.wait_send()

        if begin:

            @pl.when(jnp.logical_not(away))
            def _():
                pltpu.make_async_copy(fbuf.at[s], dst, f_recv.at[0]).start()

    def stage_a(s):
        a, b, p = blocks(s)
        if s < PIECES:
            d_arrival(p).wait_recv()
        else:
            y_arrival(p).wait_recv()
            e_copy(p).start()
            e_arrival(p).wait_recv()
        if s == 0:
            w_load.wait()
        if s >= SLOTS:
            z1_copy(s - SLOTS).wait_send()
            z2_copy(s - SLOTS).wait_send()
        slot = s % SLOTS
        pbuf[slot] = jnp.zeros(pbuf.shape[1:], jnp.float32)

        @pl.loop(0, nb // kc)
        def _(i):
            cols = pl.ds(pl.multiple_of(i * kc, kc), kc)
            lhs = jnp.concatenate([dyf[rows(a, p), cols], dyf[rows(b, p), cols]], axis=0)
            pbuf[slot] += lax.dot_general(
                lhs, wv[:, cols], (((1,), (1,)), ((), ())), preferred_element_type=jnp.float32
            )

        z1_copy(s).start()

    def stage_b(s):
        z1_copy(s).wait_recv()
        slot = s % SLOTS
        pbuf[slot, kept(1 - zh)] += rb1[s, part(1 - zh)]
        z2_copy(s).start()

    def stage_c(s):
        z2_copy(s).wait_recv()
        total = (pbuf[s % SLOTS, kept(zh)] + rb1[s, part(zh)]) + rb2[s]
        fbuf[s] = total.astype(fbuf.dtype)
        f_start(s, True)

    def o_copy(j, slot):
        cols = pl.ds(pl.multiple_of(j * nc, nc), nc)
        return pltpu.make_async_copy(obuf.at[slot], dw_ref.at[:, cols], o_sem.at[slot])

    def dw_chunks(lo, hi):
        @pl.loop(lo, hi)
        def _(j):
            slot = j % 2

            @pl.when(j >= 2)
            def _():
                o_copy(j - 2, slot).wait()

            cols = pl.ds(pl.multiple_of(j * nc, nc), nc)
            obuf[slot] = lax.dot_general(
                xf[...], dyf[:, cols], (((0,), (0,)), ((), ())), preferred_element_type=jnp.float32
            )
            o_copy(j, slot).start()

    stage_a(0)
    stage_a(1)
    x_point(0)
    stage_b(0)
    stage_a(2)
    x_point(1)
    stage_b(1)
    stage_c(0)
    stage_a(3)
    x_point(2)
    stage_b(2)
    stage_c(1)
    stage_b(3)
    stage_c(2)
    x_point(3)
    stage_c(3)
    for s in range(PIECES, STEPS - 1):
        stage_a(s)
        x_point(s)
        stage_b(s)
        stage_c(s)
    last = STEPS - 1
    chunks = nb // nc
    stage_a(last)
    cut1, cut2 = (chunks * 5) // 14, (chunks * 10) // 14
    dw_chunks(0, cut1)
    stage_b(last)
    dw_chunks(cut1, cut2)
    stage_c(last)
    dw_chunks(cut2, chunks)

    for j in (chunks - 2, chunks - 1):
        o_copy(j, j % 2).wait()
    for p in range(PIECES):
        y_copy(p).wait_send()
        d_copy(p).wait_send()
        e_copy(p).wait_send()
    for s in range(STEPS - SLOTS, STEPS):
        z1_copy(s).wait_send()
        z2_copy(s).wait_send()
    for s in range(STEPS):
        f_start(s, False)
    for t in range(4):
        @pl.when(go_right)
        def _():
            x_right_copy(t).wait_send()

        @pl.when(go_left)
        def _():
            x_left_copy(t).wait_send()

    @pl.when(r != z)
    def _():
        x_out.wait_send()

    pltpu.make_async_copy(dx_ref, dx_ref, f_recv.at[0]).wait()


def solution(mesh):
    rows = P(("data", "r"), "c")

    def local(x, w, dy):
        tb, kb = x.shape
        nb = dy.shape[1]
        pr = tb // PIECES
        nc = pick(nb, 512)
        any_spec = pl.BlockSpec(memory_space=pl.ANY)
        dma = pltpu.SemaphoreType.DMA
        return pl.pallas_call(
            kernel,
            name="linear_backward",
            out_shape=(
                jax.ShapeDtypeStruct((tb, kb), jnp.bfloat16),
                jax.ShapeDtypeStruct((kb, nb), jnp.float32),
            ),
            in_specs=[any_spec] * 3,
            out_specs=(any_spec, any_spec),
            scratch_shapes=[
                pltpu.VMEM((4 * tb, nb), jnp.bfloat16),
                pltpu.VMEM((kb, nb), jnp.bfloat16),
                pltpu.VMEM((4 * tb, kb), jnp.bfloat16),
                pltpu.VMEM((SLOTS, 2 * pr, kb), jnp.float32),
                pltpu.VMEM((STEPS, pr, kb), jnp.float32),
                pltpu.VMEM((STEPS, pr // 2, kb), jnp.float32),
                pltpu.VMEM((STEPS, pr // 2, kb), jnp.bfloat16),
                pltpu.VMEM((2, kb, nc), jnp.float32),
                dma((PIECES,)), dma,
                dma((PIECES,)), dma((PIECES,)), dma((PIECES,)), dma((PIECES,)), dma((PIECES,)), dma((PIECES,)),
                dma((STEPS,)), dma((STEPS,)), dma((STEPS,)), dma((STEPS,)), dma((STEPS,)), dma((1,)),
                dma((1,)), dma((4,)), dma((4,)), dma((4,)), dma((2,)),
            ],
            compiler_params=pltpu.CompilerParams(
                collective_id=0, has_side_effects=True, vmem_limit_bytes=67_000_000
            ),
        )(x, w, dy)

    return jax.shard_map(local, mesh=mesh, in_specs=(rows, P("r", "c"), rows), out_specs=(rows, rows), check_vma=False)
```

```python
import jax
import jax.numpy as jnp
from jax import lax
from jax.experimental import pallas as pl
from jax.experimental.pallas import tpu as pltpu
from jax.sharding import PartitionSpec as P

MESH = pl.DeviceIdType.MESH
NEAR = ((0, 2), (2, 2), (4, 2), (6, 2))
FAR = ((0, 2), (2, 2), (4, 2), (6, 1), (7, 1))
LATE = 6
STEPS = len(NEAR) + len(FAR)
SLOTS = 4


def pick(size, want):
    return want if size % want == 0 else 128


def kernel(
    x_ref, w_ref, dy_ref, dx_ref, dw_ref, xl_ref, dyl_ref,
    dyf, wv, xf, xmid, pbuf, rb1, rb2, fbuf, obuf,
    ld_sem, w_sem, y_send, y_recv, d_send, d_recv, e_send, e_recv,
    z1_send, z1_recv, z2_send, z2_recv, f_send, f_recv,
    x_src, x_recv, x_left, x_right, m_sem, o_sem, l_sem,
):
    z, r = lax.axis_index("c"), lax.axis_index("r")
    y, k = r // 2, r % 2
    mate, over, over_mate = 2 * y + 1 - k, 2 * (1 - y) + k, 2 * (1 - y) + 1 - k
    zb, zh = z % 2, z // 2
    z1, z2 = 2 * zh + 1 - zb, 2 * (1 - zh) + zb
    tb, kb = x_ref.shape
    nb = dy_ref.shape[1]
    unit = tb // 8
    kc, nc = pick(nb, 1024), pick(nb, 512)

    def rows(block, span):
        return pl.ds(pl.multiple_of(block * tb + span[0] * unit, unit), span[1] * unit)

    def send(src, dst, ssem, rsem, c=None, rr=None):
        dev = {}
        if c is not None:
            dev["c"] = c
        if rr is not None:
            dev["r"] = rr
        return pltpu.make_async_remote_copy(
            src_ref=src, dst_ref=dst, send_sem=ssem, recv_sem=rsem, device_id=dev, device_id_type=MESH
        )

    def load(p):
        src = dy_ref.at[pl.ds(NEAR[p][0] * unit, NEAR[p][1] * unit)]
        return pltpu.make_async_copy(src, dyf.at[rows(r, NEAR[p])], ld_sem.at[p])

    w_load = pltpu.make_async_copy(w_ref, wv, w_sem)
    for p in range(len(NEAR)):
        load(p).start()
    w_load.start()

    barrier = pltpu.get_barrier_semaphore()
    for i in range(1, 16):
        peer = {"c": (z + i // 4) % 4, "r": (r + i % 4) % 4}
        pl.semaphore_signal(barrier, inc=1, device_id=peer, device_id_type=MESH)
    pl.semaphore_wait(barrier, 15)

    def xrows(t):
        return pl.ds(pl.multiple_of(t * tb, tb), tb)

    detour = jnp.logical_and(k == 1, y != zh)
    relay = jnp.logical_and(k == 1, y == zh)
    direct = jnp.logical_and(jnp.logical_not(detour), r != z)
    x_own = pltpu.make_async_copy(x_ref, xf.at[xrows(r)], x_recv.at[r])
    x_out = send(x_ref, xf.at[xrows(r)], x_src.at[0], x_recv.at[r], c=z, rr=z)
    m_out = send(x_ref, xmid, m_sem.at[0], m_sem.at[1], c=z2)
    m_pass = send(xmid, xf.at[xrows(r)], m_sem.at[2], x_recv.at[r], c=z, rr=z2)

    @pl.when(r == z)
    def _():
        x_own.start()

    @pl.when(direct)
    def _():
        x_out.start()

    @pl.when(detour)
    def _():
        m_out.start()

    def y_copy(p):
        return send(dyf.at[rows(r, FAR[p])], dyf.at[rows(r, FAR[p])], y_send.at[p], y_recv.at[p], rr=over)

    def d_copy(p):
        return send(dyf.at[rows(r, NEAR[p])], dyf.at[rows(r, NEAR[p])], d_send.at[p], d_recv.at[p], rr=mate)

    def e_copy(p):
        return send(dyf.at[rows(over, FAR[p])], dyf.at[rows(over, FAR[p])], e_send.at[p], e_recv.at[p], rr=mate)

    def y_arrival(p):
        return send(dyf.at[rows(over, FAR[p])], dyf.at[rows(over, FAR[p])], y_send.at[p], y_recv.at[p], rr=over)

    def d_arrival(p):
        return send(dyf.at[rows(mate, NEAR[p])], dyf.at[rows(mate, NEAR[p])], d_send.at[p], d_recv.at[p], rr=mate)

    def e_arrival(p):
        at = rows(over_mate, FAR[p])
        return send(dyf.at[at], dyf.at[at], e_send.at[p], e_recv.at[p], rr=mate)

    for p in range(len(NEAR)):
        load(p).wait()
        if p == 0:
            y_copy(0).start()
        d_copy(p).start()

    def y_rest():
        @pl.when(relay)
        def _():
            m_out.wait_recv()
            m_pass.start()

        for p in range(1, len(FAR)):
            y_copy(p).start()

    def x_route(t):
        near = y == t // 2
        head = jnp.where(jnp.logical_or(near, t % 2 == 0), r, (r + 2) % 4)
        hops = jnp.where(z >= head, z - head, head - z)
        turn = jnp.where(near, t % 2, 2 + t % 2)
        go_right = jnp.logical_and(z >= head, z < 3)
        go_left = jnp.logical_and(z <= head, z > 0)
        return turn + hops, go_right, go_left

    routes = [x_route(t) for t in range(4)]

    def x_right_copy(t):
        return send(xf.at[xrows(t)], xf.at[xrows(t)], x_right.at[t], x_recv.at[t], c=z + 1)

    def x_left_copy(t):
        return send(xf.at[xrows(t)], xf.at[xrows(t)], x_left.at[t], x_recv.at[t], c=z - 1)

    def x_point(j):
        for t in range(4):
            when, go_right, go_left = routes[t]
            live = when == j

            @pl.when(live)
            def _():
                pltpu.make_async_copy(x_ref, xf.at[xrows(t)], x_recv.at[t]).wait()

            @pl.when(jnp.logical_and(live, go_right))
            def _():
                x_right_copy(t).start()

            @pl.when(jnp.logical_and(live, go_left))
            def _():
                x_left_copy(t).start()

    def blocks(s):
        return (r, mate, NEAR[s]) if s < len(NEAR) else (over, over_mate, FAR[s - len(NEAR)])

    def size(s):
        return blocks(s)[2][1] * unit

    def z1_copy(s):
        n = size(s)
        half = pl.ds(pl.multiple_of((1 - zb) * n, n), n)
        return send(pbuf.at[s % SLOTS, half], rb1.at[s, pl.ds(0, n)], z1_send.at[s], z1_recv.at[s], c=z1)

    def kept(s, i):
        n = size(s) // 2
        return pl.ds(pl.multiple_of(zb * 2 * n + i * n, n), n)

    def part(s, i):
        n = size(s) // 2
        return pl.ds(pl.multiple_of(i * n, n), n)

    def z2_copy(s):
        dst = rb2.at[s, pl.ds(0, size(s) // 2)]
        return send(pbuf.at[s % SLOTS, kept(s, 1 - zh)], dst, z2_send.at[s], z2_recv.at[s], c=z2)

    def f_start(s, begin):
        a, b, span = blocks(s)
        n = size(s) // 2
        owner = a + zb * (b - a)
        src = fbuf.at[s, pl.ds(0, n)]
        dst = dx_ref.at[pl.ds(pl.multiple_of(span[0] * unit + zh * n, n), n)]
        away = jnp.logical_or(z != r, owner != r)

        @pl.when(away)
        def _():
            copy = send(src, dst, f_send.at[s], f_recv.at[0], c=r, rr=owner)
            copy.start() if begin else copy.wait_send()

        if begin:

            @pl.when(jnp.logical_not(away))
            def _():
                pltpu.make_async_copy(src, dst, f_recv.at[0]).start()

    def stage_a(s):
        a, b, span = blocks(s)
        p = s - len(NEAR)
        if p < 0:
            d_arrival(s).wait_recv()
        else:
            y_arrival(p).wait_recv()
            e_copy(p).start()
            e_arrival(p).wait_recv()
        if s == 0:
            w_load.wait()
        if s >= SLOTS:
            z1_copy(s - SLOTS).wait_send()
            z2_copy(s - SLOTS).wait_send()
        slot, n = s % SLOTS, 2 * size(s)
        pbuf[slot, :n] = jnp.zeros((n, kb), jnp.float32)

        @pl.loop(0, nb // kc)
        def _(i):
            cols = pl.ds(pl.multiple_of(i * kc, kc), kc)
            lhs = jnp.concatenate([dyf[rows(a, span), cols], dyf[rows(b, span), cols]], axis=0)
            pbuf[slot, :n] += lax.dot_general(
                lhs, wv[:, cols], (((1,), (1,)), ((), ())), preferred_element_type=jnp.float32
            )

        z1_copy(s).start()

    def stage_b(s):
        z1_copy(s).wait_recv()
        pbuf[s % SLOTS, kept(s, 1 - zh)] += rb1[s, part(s, 1 - zh)]
        z2_copy(s).start()

    def stage_c(s):
        z2_copy(s).wait_recv()
        n = size(s) // 2
        total = (pbuf[s % SLOTS, kept(s, zh)] + rb1[s, part(s, zh)]) + rb2[s, :n]
        fbuf[s, :n] = total.astype(fbuf.dtype)
        f_start(s, True)

    def o_copy(j, slot):
        cols = pl.ds(pl.multiple_of(j * nc, nc), nc)
        return pltpu.make_async_copy(obuf.at[slot], dw_ref.at[:, cols], o_sem.at[slot])

    early = [pl.ds(pl.multiple_of(y * 2 * tb, 2 * tb), 2 * tb), rows(2 * (1 - y), (0, LATE)), rows(3 - 2 * y, (0, LATE))]

    def dw_early():
        @pl.loop(0, nb // nc)
        def _(j):
            slot = j % 2

            @pl.when(j >= 2)
            def _():
                o_copy(j - 2, slot).wait()

            cols = pl.ds(pl.multiple_of(j * nc, nc), nc)
            terms = [
                lax.dot_general(xf[at], dyf[at, cols], (((0,), (0,)), ((), ())), preferred_element_type=jnp.float32)
                for at in early
            ]
            obuf[slot] = (terms[0] + terms[1]) + terms[2]
            o_copy(j, slot).start()

    late = (8 - LATE) * unit

    def x_late(i):
        src = xf.at[rows((over, over_mate)[i], (LATE, 8 - LATE))]
        return pltpu.make_async_copy(src, xl_ref.at[pl.ds(i * late, late)], l_sem.at[i])

    def dy_late(i):
        src = dyf.at[rows((over, over_mate)[i], (LATE, 8 - LATE))]
        return pltpu.make_async_copy(src, dyl_ref.at[pl.ds(i * late, late)], l_sem.at[2 + i])

    stage_a(0)
    stage_a(1)
    y_rest()
    x_point(0)
    stage_b(0)
    stage_a(2)
    x_point(1)
    stage_b(1)
    stage_c(0)
    stage_a(3)
    x_point(2)
    stage_b(2)
    stage_c(1)
    stage_b(3)
    stage_c(2)
    stage_c(3)
    stage_a(4)
    x_point(3)
    stage_b(4)
    stage_c(4)
    x_point(4)
    stage_a(5)
    x_point(5)
    stage_b(5)
    stage_c(5)
    x_point(6)
    x_late(0).start()
    x_late(1).start()
    stage_a(6)
    stage_b(6)
    stage_c(6)
    dw_early()
    stage_a(7)
    stage_b(7)
    stage_c(7)
    stage_a(8)
    dy_late(0).start()
    dy_late(1).start()
    stage_b(8)
    stage_c(8)

    chunks = nb // nc
    for j in (chunks - 2, chunks - 1):
        o_copy(j, j % 2).wait()
    for p in range(len(NEAR)):
        d_copy(p).wait_send()
    for p in range(len(FAR)):
        y_copy(p).wait_send()
        e_copy(p).wait_send()
    for s in range(STEPS - SLOTS, STEPS):
        z1_copy(s).wait_send()
        z2_copy(s).wait_send()
    for s in range(STEPS):
        f_start(s, False)
    for t in range(4):
        _, go_right, go_left = routes[t]

        @pl.when(go_right)
        def _():
            x_right_copy(t).wait_send()

        @pl.when(go_left)
        def _():
            x_left_copy(t).wait_send()

    @pl.when(direct)
    def _():
        x_out.wait_send()

    @pl.when(detour)
    def _():
        m_out.wait_send()

    @pl.when(relay)
    def _():
        m_pass.wait_send()

    for i in range(2):
        x_late(i).wait()
        dy_late(i).wait()
    pltpu.make_async_copy(dx_ref, dx_ref, f_recv.at[0]).wait()


def solution(mesh):
    rows = P(("data", "r"), "c")

    def local(x, w, dy):
        tb, kb = x.shape
        nb = dy.shape[1]
        pr, late = tb // 4, 2 * tb * (8 - LATE) // 8
        nc = pick(nb, 512)
        any_spec = pl.BlockSpec(memory_space=pl.ANY)
        dma = pltpu.SemaphoreType.DMA
        far, steps = (len(FAR),), (STEPS,)
        dx, dw_early, x_late, dy_late = pl.pallas_call(
            kernel,
            name="linear_backward",
            out_shape=(
                jax.ShapeDtypeStruct((tb, kb), jnp.bfloat16),
                jax.ShapeDtypeStruct((kb, nb), jnp.float32),
                jax.ShapeDtypeStruct((late, kb), jnp.bfloat16),
                jax.ShapeDtypeStruct((late, nb), jnp.bfloat16),
            ),
            in_specs=[any_spec] * 3,
            out_specs=(any_spec,) * 4,
            scratch_shapes=[
                pltpu.VMEM((4 * tb, nb), jnp.bfloat16),
                pltpu.VMEM((kb, nb), jnp.bfloat16),
                pltpu.VMEM((4 * tb, kb), jnp.bfloat16),
                pltpu.VMEM((tb, kb), jnp.bfloat16),
                pltpu.VMEM((SLOTS, 2 * pr, kb), jnp.float32),
                pltpu.VMEM((STEPS, pr, kb), jnp.float32),
                pltpu.VMEM((STEPS, pr // 2, kb), jnp.float32),
                pltpu.VMEM((STEPS, pr // 2, kb), jnp.bfloat16),
                pltpu.VMEM((2, kb, nc), jnp.float32),
                dma((len(NEAR),)), dma, dma(far), dma(far), dma((len(NEAR),)), dma((len(NEAR),)), dma(far), dma(far),
                dma(steps), dma(steps), dma(steps), dma(steps), dma(steps), dma((1,)),
                dma((1,)), dma((4,)), dma((4,)), dma((4,)), dma((3,)), dma((2,)), dma((4,)),
            ],
            compiler_params=pltpu.CompilerParams(
                collective_id=0, has_side_effects=True, vmem_limit_bytes=67_000_000
            ),
        )(x, w, dy)
        dw_late = lax.dot_general(x_late, dy_late, (((0,), (0,)), ((), ())), preferred_element_type=jnp.float32)
        return dx, dw_early + dw_late

    return jax.shard_map(local, mesh=mesh, in_specs=(rows, P("r", "c"), rows), out_specs=(rows, rows), check_vma=False)
```

```python
import jax
import jax.numpy as jnp
from jax import lax
from jax.experimental import pallas as pl
from jax.experimental.pallas import tpu as pltpu
from jax.sharding import PartitionSpec as P

MESH = pl.DeviceIdType.MESH
NEAR = ((0, 2), (2, 2), (4, 2), (6, 2))
FAR = ((0, 2), (2, 2), (4, 2), (6, 1), (7, 1))
LATE = 4
STEPS = len(NEAR) + len(FAR)
SLOTS = 4


def pick(size, want):
    return want if size % want == 0 else 128


def kernel(
    x_ref, w_ref, dy_ref, dx_ref, dw_ref, xl_ref, dyl_ref,
    dyf, wv, xf, xmid, pbuf, rb1, rb2, fbuf, obuf,
    ld_sem, w_sem, y_send, y_recv, d_send, d_recv, e_send, e_recv,
    z1_send, z1_recv, z2_send, z3_send, z2_recv, f_send, f_recv,
    x_src, x_recv, x_left, x_right, m_sem, o_sem, l_sem,
):
    z, r = lax.axis_index("c"), lax.axis_index("r")
    y, k = r // 2, r % 2
    mate, over, over_mate = 2 * y + 1 - k, 2 * (1 - y) + k, 2 * (1 - y) + 1 - k
    zb, zh = z % 2, z // 2
    z1, z2 = 2 * zh + 1 - zb, 2 * (1 - zh) + zb
    tb, kb = x_ref.shape
    nb = dy_ref.shape[1]
    unit = tb // 8
    kc, nc = pick(nb, 1024), pick(nb, 512)

    def rows(block, span):
        return pl.ds(pl.multiple_of(block * tb + span[0] * unit, unit), span[1] * unit)

    def send(src, dst, ssem, rsem, c=None, rr=None):
        dev = {}
        if c is not None:
            dev["c"] = c
        if rr is not None:
            dev["r"] = rr
        return pltpu.make_async_remote_copy(
            src_ref=src, dst_ref=dst, send_sem=ssem, recv_sem=rsem, device_id=dev, device_id_type=MESH
        )

    def load(p):
        src = dy_ref.at[pl.ds(NEAR[p][0] * unit, NEAR[p][1] * unit)]
        return pltpu.make_async_copy(src, dyf.at[rows(r, NEAR[p])], ld_sem.at[p])

    w_load = pltpu.make_async_copy(w_ref, wv, w_sem)
    for p in range(len(NEAR)):
        load(p).start()
    w_load.start()

    barrier = pltpu.get_barrier_semaphore()
    for i in range(1, 16):
        peer = {"c": (z + i // 4) % 4, "r": (r + i % 4) % 4}
        pl.semaphore_signal(barrier, inc=1, device_id=peer, device_id_type=MESH)
    pl.semaphore_wait(barrier, 15)

    def xrows(t):
        return pl.ds(pl.multiple_of(t * tb, tb), tb)

    detour = jnp.logical_and(k == 1, y != zh)
    relay = jnp.logical_and(k == 1, y == zh)
    direct = jnp.logical_and(jnp.logical_not(detour), r != z)
    x_own = pltpu.make_async_copy(x_ref, xf.at[xrows(r)], x_recv.at[r])
    x_out = send(x_ref, xf.at[xrows(r)], x_src.at[0], x_recv.at[r], c=z, rr=z)
    m_out = send(x_ref, xmid, m_sem.at[0], m_sem.at[1], c=z2)
    m_pass = send(xmid, xf.at[xrows(r)], m_sem.at[2], x_recv.at[r], c=z, rr=z2)

    @pl.when(r == z)
    def _():
        x_own.start()

    @pl.when(direct)
    def _():
        x_out.start()

    @pl.when(detour)
    def _():
        m_out.start()

    def y_copy(p):
        return send(dyf.at[rows(r, FAR[p])], dyf.at[rows(r, FAR[p])], y_send.at[p], y_recv.at[p], rr=over)

    def d_copy(p):
        return send(dyf.at[rows(r, NEAR[p])], dyf.at[rows(r, NEAR[p])], d_send.at[p], d_recv.at[p], rr=mate)

    def e_copy(p):
        return send(dyf.at[rows(over, FAR[p])], dyf.at[rows(over, FAR[p])], e_send.at[p], e_recv.at[p], rr=mate)

    def y_arrival(p):
        return send(dyf.at[rows(over, FAR[p])], dyf.at[rows(over, FAR[p])], y_send.at[p], y_recv.at[p], rr=over)

    def d_arrival(p):
        return send(dyf.at[rows(mate, NEAR[p])], dyf.at[rows(mate, NEAR[p])], d_send.at[p], d_recv.at[p], rr=mate)

    def e_arrival(p):
        at = rows(over_mate, FAR[p])
        return send(dyf.at[at], dyf.at[at], e_send.at[p], e_recv.at[p], rr=mate)

    for p in range(len(NEAR)):
        load(p).wait()
        if p == 0:
            y_copy(0).start()
        d_copy(p).start()

    def y_rest():
        @pl.when(relay)
        def _():
            m_out.wait_recv()
            m_pass.start()

        for p in range(1, len(FAR)):
            y_copy(p).start()

    def x_route(t):
        near = y == t // 2
        head = jnp.where(jnp.logical_or(near, t % 2 == 0), r, (r + 2) % 4)
        hops = jnp.where(z >= head, z - head, head - z)
        turn = jnp.where(near, t % 2, 2 + t % 2)
        go_right = jnp.logical_and(z >= head, z < 3)
        go_left = jnp.logical_and(z <= head, z > 0)
        return turn + hops, go_right, go_left

    routes = [x_route(t) for t in range(4)]

    def x_right_copy(t):
        return send(xf.at[xrows(t)], xf.at[xrows(t)], x_right.at[t], x_recv.at[t], c=z + 1)

    def x_left_copy(t):
        return send(xf.at[xrows(t)], xf.at[xrows(t)], x_left.at[t], x_recv.at[t], c=z - 1)

    def x_point(j):
        for t in range(4):
            when, go_right, go_left = routes[t]
            live = when == j

            @pl.when(live)
            def _():
                pltpu.make_async_copy(x_ref, xf.at[xrows(t)], x_recv.at[t]).wait()

            @pl.when(jnp.logical_and(live, go_right))
            def _():
                x_right_copy(t).start()

            @pl.when(jnp.logical_and(live, go_left))
            def _():
                x_left_copy(t).start()

    def blocks(s):
        return (r, mate, NEAR[s]) if s < len(NEAR) else (over, over_mate, FAR[s - len(NEAR)])

    def size(s):
        return blocks(s)[2][1] * unit

    inner = jnp.logical_or(z == 1, z == 2)
    end = jnp.logical_not(inner)
    far_end = 3 * (1 - zh)

    def at(first, n, count=1):
        return pl.ds(pl.multiple_of(first * n, n), count * n)

    def z1_end(s):
        n = size(s) // 2
        src = pbuf.at[s % SLOTS, at(1 - zh, n, 3)]
        return send(src, rb1.at[s, pl.ds(0, 3 * n)], z1_send.at[s], z1_recv.at[s], c=z1)

    def z1_inner(s):
        n = size(s) // 2
        src = pbuf.at[s % SLOTS, at(3 * zh, n)]
        return send(src, rb1.at[s, pl.ds(0, n)], z1_send.at[s], z1_recv.at[s], c=z1)

    def z2_copy(s):
        n = size(s) // 2
        return send(pbuf.at[s % SLOTS, at(3 - z, n)], rb2.at[s, pl.ds(0, n)], z2_send.at[s], z2_recv.at[s], c=3 - z)

    def z3_copy(s):
        n = size(s) // 2
        src = pbuf.at[s % SLOTS, at(far_end, n)]
        return send(src, rb2.at[s, pl.ds(0, n)], z3_send.at[s], z2_recv.at[s], c=far_end)

    def z_sent(s):
        @pl.when(end)
        def _():
            z1_end(s).wait_send()

        @pl.when(inner)
        def _():
            z1_inner(s).wait_send()
            z2_copy(s).wait_send()
            z3_copy(s).wait_send()

    def f_start(s, begin):
        a, b, span = blocks(s)
        n = size(s) // 2
        owner = a + zh * (b - a)
        src = fbuf.at[s, pl.ds(0, n)]
        dst = dx_ref.at[pl.ds(pl.multiple_of(span[0] * unit + zb * n, n), n)]
        away = jnp.logical_or(z != r, owner != r)

        @pl.when(away)
        def _():
            copy = send(src, dst, f_send.at[s], f_recv.at[0], c=r, rr=owner)
            copy.start() if begin else copy.wait_send()

        if begin:

            @pl.when(jnp.logical_not(away))
            def _():
                pltpu.make_async_copy(src, dst, f_recv.at[0]).start()

    def stage_a(s):
        a, b, span = blocks(s)
        p = s - len(NEAR)
        if p < 0:
            with jax.named_scope(f"wd{s}"):
                d_arrival(s).wait_recv()
        else:
            with jax.named_scope(f"wy{s}"):
                y_arrival(p).wait_recv()
            e_copy(p).start()
            with jax.named_scope(f"we{s}"):
                e_arrival(p).wait_recv()
        if s == 0:
            w_load.wait()
        if s >= SLOTS:
            z_sent(s - SLOTS)
        slot, n = s % SLOTS, 2 * size(s)
        pbuf[slot, :n] = jnp.zeros((n, kb), jnp.float32)

        @pl.loop(0, nb // kc)
        def _(i):
            cols = pl.ds(pl.multiple_of(i * kc, kc), kc)
            lhs = jnp.concatenate([dyf[rows(a, span), cols], dyf[rows(b, span), cols]], axis=0)
            pbuf[slot, :n] += lax.dot_general(
                lhs, wv[:, cols], (((1,), (1,)), ((), ())), preferred_element_type=jnp.float32
            )

        @pl.when(end)
        def _():
            z1_end(s).start()

        @pl.when(inner)
        def _():
            z1_inner(s).start()

    def stage_b(s):
        n = size(s) // 2

        @pl.when(inner)
        def _():
            z1_end(s).wait_recv()
            pbuf[s % SLOTS, at(2 * (1 - zh), n, 2)] += rb1[s, at(1 - zh, n, 2)]
            z3_copy(s).start()
            z2_copy(s).start()

    def stage_c(s):
        n = size(s) // 2

        @pl.when(end)
        def _():
            z1_inner(s).wait_recv()

        z2_copy(s).wait_recv()
        mine = jnp.where(inner, 2 * zh, 0)
        total = (pbuf[s % SLOTS, at(z, n)] + rb1[s, at(mine, n)]) + rb2[s, :n]
        fbuf[s, :n] = total.astype(fbuf.dtype)
        f_start(s, True)

    def o_copy(j, slot):
        cols = pl.ds(pl.multiple_of(j * nc, nc), nc)
        return pltpu.make_async_copy(obuf.at[slot], dw_ref.at[:, cols], o_sem.at[slot])

    early = [pl.ds(pl.multiple_of(y * 2 * tb, 2 * tb), 2 * tb), rows(2 * (1 - y), (0, LATE)), rows(3 - 2 * y, (0, LATE))]

    def dw_early(lo, hi):
        chunks = nb // nc

        @pl.loop((lo * chunks) // 14, (hi * chunks) // 14)
        def _(j):
            slot = j % 2

            @pl.when(j >= 2)
            def _():
                o_copy(j - 2, slot).wait()

            cols = pl.ds(pl.multiple_of(j * nc, nc), nc)
            terms = [
                lax.dot_general(xf[at], dyf[at, cols], (((0,), (0,)), ((), ())), preferred_element_type=jnp.float32)
                for at in early
            ]
            obuf[slot] = (terms[0] + terms[1]) + terms[2]
            o_copy(j, slot).start()

    late = (8 - LATE) * unit

    def x_late(i):
        src = xf.at[rows((over, over_mate)[i], (LATE, 8 - LATE))]
        return pltpu.make_async_copy(src, xl_ref.at[pl.ds(i * late, late)], l_sem.at[i])

    def dy_late(i):
        src = dyf.at[rows((over, over_mate)[i], (LATE, 8 - LATE))]
        return pltpu.make_async_copy(src, dyl_ref.at[pl.ds(i * late, late)], l_sem.at[2 + i])

    with jax.named_scope("a0"):
        stage_a(0)
    with jax.named_scope("x0"):
        x_point(0)
    with jax.named_scope("a1"):
        stage_a(1)
    with jax.named_scope("y_rest"):
        y_rest()
    with jax.named_scope("a2"):
        stage_a(2)
    with jax.named_scope("a3"):
        stage_a(3)
    with jax.named_scope("b0"):
        stage_b(0)
    with jax.named_scope("b1"):
        stage_b(1)
    with jax.named_scope("c0"):
        stage_c(0)
    with jax.named_scope("x1"):
        x_point(1)
    with jax.named_scope("b2"):
        stage_b(2)
    with jax.named_scope("c1"):
        stage_c(1)
    with jax.named_scope("b3"):
        stage_b(3)
    with jax.named_scope("c2"):
        stage_c(2)
    with jax.named_scope("c3"):
        stage_c(3)
    with jax.named_scope("x2"):
        x_point(2)
    with jax.named_scope("a4"):
        stage_a(4)
    with jax.named_scope("b4"):
        stage_b(4)
    with jax.named_scope("x3"):
        x_point(3)
    with jax.named_scope("c4"):
        stage_c(4)
    with jax.named_scope("a5"):
        stage_a(5)
    with jax.named_scope("x4"):
        x_point(4)
    with jax.named_scope("b5"):
        stage_b(5)
    with jax.named_scope("c5"):
        stage_c(5)
    with jax.named_scope("x5"):
        x_point(5)
    with jax.named_scope("a6"):
        stage_a(6)
    with jax.named_scope("b6"):
        stage_b(6)
    with jax.named_scope("x6"):
        x_point(6)
    with jax.named_scope("c6"):
        stage_c(6)
    x_late(0).start()
    x_late(1).start()
    with jax.named_scope("dw0_3"):
        dw_early(0, 3)
    with jax.named_scope("a7"):
        stage_a(7)
    with jax.named_scope("b7"):
        stage_b(7)
    with jax.named_scope("dw3_6"):
        dw_early(3, 6)
    with jax.named_scope("c7"):
        stage_c(7)
    with jax.named_scope("a8"):
        stage_a(8)
    dy_late(0).start()
    dy_late(1).start()
    with jax.named_scope("dw6_10"):
        dw_early(6, 10)
    with jax.named_scope("b8"):
        stage_b(8)
    with jax.named_scope("dw10_14"):
        dw_early(10, 14)
    with jax.named_scope("c8"):
        stage_c(8)

    chunks = nb // nc
    for j in (chunks - 2, chunks - 1):
        o_copy(j, j % 2).wait()
    for p in range(len(NEAR)):
        d_copy(p).wait_send()
    for p in range(len(FAR)):
        y_copy(p).wait_send()
        e_copy(p).wait_send()
    for s in range(STEPS - SLOTS, STEPS):
        z_sent(s)
    for s in range(STEPS):
        f_start(s, False)
    for t in range(4):
        _, go_right, go_left = routes[t]

        @pl.when(go_right)
        def _():
            x_right_copy(t).wait_send()

        @pl.when(go_left)
        def _():
            x_left_copy(t).wait_send()

    @pl.when(direct)
    def _():
        x_out.wait_send()

    @pl.when(detour)
    def _():
        m_out.wait_send()

    @pl.when(relay)
    def _():
        m_pass.wait_send()

    for i in range(2):
        x_late(i).wait()
        dy_late(i).wait()
    pltpu.make_async_copy(dx_ref, dx_ref, f_recv.at[0]).wait()


def solution(mesh):
    rows = P(("data", "r"), "c")

    def local(x, w, dy):
        tb, kb = x.shape
        nb = dy.shape[1]
        pr, late = tb // 4, 2 * tb * (8 - LATE) // 8
        nc = pick(nb, 512)
        any_spec = pl.BlockSpec(memory_space=pl.ANY)
        dma = pltpu.SemaphoreType.DMA
        far, steps = (len(FAR),), (STEPS,)
        dx, dw_early, x_late, dy_late = pl.pallas_call(
            kernel,
            name="linear_backward",
            out_shape=(
                jax.ShapeDtypeStruct((tb, kb), jnp.bfloat16),
                jax.ShapeDtypeStruct((kb, nb), jnp.float32),
                jax.ShapeDtypeStruct((late, kb), jnp.bfloat16),
                jax.ShapeDtypeStruct((late, nb), jnp.bfloat16),
            ),
            in_specs=[any_spec] * 3,
            out_specs=(any_spec,) * 4,
            scratch_shapes=[
                pltpu.VMEM((4 * tb, nb), jnp.bfloat16),
                pltpu.VMEM((kb, nb), jnp.bfloat16),
                pltpu.VMEM((4 * tb, kb), jnp.bfloat16),
                pltpu.VMEM((tb, kb), jnp.bfloat16),
                pltpu.VMEM((SLOTS, 2 * pr, kb), jnp.float32),
                pltpu.VMEM((STEPS, 3 * pr // 2, kb), jnp.float32),
                pltpu.VMEM((STEPS, pr // 2, kb), jnp.float32),
                pltpu.VMEM((STEPS, pr // 2, kb), jnp.bfloat16),
                pltpu.VMEM((2, kb, nc), jnp.float32),
                dma((len(NEAR),)), dma, dma(far), dma(far), dma((len(NEAR),)), dma((len(NEAR),)), dma(far), dma(far),
                dma(steps), dma(steps), dma(steps), dma(steps), dma(steps), dma(steps), dma((1,)),
                dma((1,)), dma((4,)), dma((4,)), dma((4,)), dma((3,)), dma((2,)), dma((4,)),
            ],
            compiler_params=pltpu.CompilerParams(
                collective_id=0, has_side_effects=True, vmem_limit_bytes=67_000_000
            ),
        )(x, w, dy)
        dw_late = lax.dot_general(x_late, dy_late, (((0,), (0,)), ((), ())), preferred_element_type=jnp.float32)
        return dx, dw_early + dw_late

    return jax.shard_map(local, mesh=mesh, in_specs=(rows, P("r", "c"), rows), out_specs=(rows, rows), check_vma=False)
```

```python
import jax
import jax.numpy as jnp
from jax import lax
from jax.experimental import pallas as pl
from jax.experimental.pallas import tpu as pltpu
from jax.sharding import PartitionSpec as P

MESH = pl.DeviceIdType.MESH
NEAR = ((0, 2), (2, 2), (4, 2), (6, 2))
FAR = ((0, 2), (2, 2), (4, 2), (6, 1), (7, 1))
LATE = 4
STEPS = len(NEAR) + len(FAR)
SLOTS = 4


def pick(size, want):
    return want if size % want == 0 else 128


def kernel(
    x_ref, w_ref, dy_ref, dx_ref, dw_ref, xl_ref, dyl_ref,
    dyf, wv, xf, xmid, pbuf, rb1, rb2, fbuf, obuf,
    ld_sem, w_sem, y_send, y_recv, d_send, d_recv, e_send, e_recv,
    z1_send, z1_recv, z2_send, z3_send, z2_recv, f_send, f_recv,
    x_src, x_recv, x_left, x_right, m_sem, o_sem, l_sem,
):
    z, r = lax.axis_index("c"), lax.axis_index("r")
    y, k = r // 2, r % 2
    mate, over, over_mate = 2 * y + 1 - k, 2 * (1 - y) + k, 2 * (1 - y) + 1 - k
    zb, zh = z % 2, z // 2
    z1, z2 = 2 * zh + 1 - zb, 2 * (1 - zh) + zb
    tb, kb = x_ref.shape
    nb = dy_ref.shape[1]
    unit = tb // 8
    kc, nc = pick(nb, 1024), pick(nb, 512)

    def rows(block, span):
        return pl.ds(pl.multiple_of(block * tb + span[0] * unit, unit), span[1] * unit)

    def send(src, dst, ssem, rsem, c=None, rr=None):
        dev = {}
        if c is not None:
            dev["c"] = c
        if rr is not None:
            dev["r"] = rr
        return pltpu.make_async_remote_copy(
            src_ref=src, dst_ref=dst, send_sem=ssem, recv_sem=rsem, device_id=dev, device_id_type=MESH
        )

    def load(p):
        src = dy_ref.at[pl.ds(NEAR[p][0] * unit, NEAR[p][1] * unit)]
        return pltpu.make_async_copy(src, dyf.at[rows(r, NEAR[p])], ld_sem.at[p])

    w_load = pltpu.make_async_copy(w_ref, wv, w_sem)
    for p in range(len(NEAR)):
        load(p).start()
    w_load.start()

    barrier = pltpu.get_barrier_semaphore()
    for i in range(1, 16):
        peer = {"c": (z + i // 4) % 4, "r": (r + i % 4) % 4}
        pl.semaphore_signal(barrier, inc=1, device_id=peer, device_id_type=MESH)
    pl.semaphore_wait(barrier, 15)

    def xrows(t):
        return pl.ds(pl.multiple_of(t * tb, tb), tb)

    detour = jnp.logical_and(k == 1, y != zh)
    relay = jnp.logical_and(k == 1, y == zh)
    direct = jnp.logical_and(jnp.logical_not(detour), r != z)
    x_own = pltpu.make_async_copy(x_ref, xf.at[xrows(r)], x_recv.at[r])
    x_out = send(x_ref, xf.at[xrows(r)], x_src.at[0], x_recv.at[r], c=z, rr=z)
    m_out = send(x_ref, xmid, m_sem.at[0], m_sem.at[1], c=z2)
    m_pass = send(xmid, xf.at[xrows(r)], m_sem.at[2], x_recv.at[r], c=z, rr=z2)

    @pl.when(r == z)
    def _():
        x_own.start()

    @pl.when(direct)
    def _():
        x_out.start()

    @pl.when(detour)
    def _():
        m_out.start()

    def y_copy(p):
        return send(dyf.at[rows(r, FAR[p])], dyf.at[rows(r, FAR[p])], y_send.at[p], y_recv.at[p], rr=over)

    def d_copy(p):
        return send(dyf.at[rows(r, NEAR[p])], dyf.at[rows(r, NEAR[p])], d_send.at[p], d_recv.at[p], rr=mate)

    def e_copy(p):
        return send(dyf.at[rows(over, FAR[p])], dyf.at[rows(over, FAR[p])], e_send.at[p], e_recv.at[p], rr=mate)

    def y_arrival(p):
        return send(dyf.at[rows(over, FAR[p])], dyf.at[rows(over, FAR[p])], y_send.at[p], y_recv.at[p], rr=over)

    def d_arrival(p):
        return send(dyf.at[rows(mate, NEAR[p])], dyf.at[rows(mate, NEAR[p])], d_send.at[p], d_recv.at[p], rr=mate)

    def e_arrival(p):
        at = rows(over_mate, FAR[p])
        return send(dyf.at[at], dyf.at[at], e_send.at[p], e_recv.at[p], rr=mate)

    for p in range(len(NEAR)):
        load(p).wait()
        if p == 0:
            y_copy(0).start()
        d_copy(p).start()

    def y_rest():
        @pl.when(relay)
        def _():
            m_out.wait_recv()
            m_pass.start()

        for p in range(1, len(FAR)):
            y_copy(p).start()

    def x_route(t):
        near = y == t // 2
        head = jnp.where(jnp.logical_or(near, t % 2 == 0), r, (r + 2) % 4)
        hops = jnp.where(z >= head, z - head, head - z)
        turn = jnp.where(near, t % 2, 2 + 2 * (t % 2))
        go_right = jnp.logical_and(z >= head, z < 3)
        go_left = jnp.logical_and(z <= head, z > 0)
        return turn + hops, go_right, go_left

    routes = [x_route(t) for t in range(4)]

    def x_right_copy(t):
        return send(xf.at[xrows(t)], xf.at[xrows(t)], x_right.at[t], x_recv.at[t], c=z + 1)

    def x_left_copy(t):
        return send(xf.at[xrows(t)], xf.at[xrows(t)], x_left.at[t], x_recv.at[t], c=z - 1)

    def x_point(j):
        for t in range(4):
            when, go_right, go_left = routes[t]
            live = when == j

            @pl.when(live)
            def _():
                pltpu.make_async_copy(x_ref, xf.at[xrows(t)], x_recv.at[t]).wait()

            @pl.when(jnp.logical_and(live, go_right))
            def _():
                x_right_copy(t).start()

            @pl.when(jnp.logical_and(live, go_left))
            def _():
                x_left_copy(t).start()

    def blocks(s):
        return (r, mate, NEAR[s]) if s < len(NEAR) else (over, over_mate, FAR[s - len(NEAR)])

    def size(s):
        return blocks(s)[2][1] * unit

    inner = jnp.logical_or(z == 1, z == 2)
    end = jnp.logical_not(inner)
    far_end = 3 * (1 - zh)

    def at(first, n, count=1):
        return pl.ds(pl.multiple_of(first * n, n), count * n)

    def z1_end(s):
        n = size(s) // 2
        src = pbuf.at[s % SLOTS, at(1 - zh, n, 3)]
        return send(src, rb1.at[s, pl.ds(0, 3 * n)], z1_send.at[s], z1_recv.at[s], c=z1)

    def z1_inner(s):
        n = size(s) // 2
        src = pbuf.at[s % SLOTS, at(3 * zh, n)]
        return send(src, rb1.at[s, pl.ds(0, n)], z1_send.at[s], z1_recv.at[s], c=z1)

    def z2_copy(s):
        n = size(s) // 2
        return send(pbuf.at[s % SLOTS, at(3 - z, n)], rb2.at[s, pl.ds(0, n)], z2_send.at[s], z2_recv.at[s], c=3 - z)

    def z3_copy(s):
        n = size(s) // 2
        src = pbuf.at[s % SLOTS, at(far_end, n)]
        return send(src, rb2.at[s, pl.ds(0, n)], z3_send.at[s], z2_recv.at[s], c=far_end)

    def z_sent(s):
        @pl.when(end)
        def _():
            z1_end(s).wait_send()

        @pl.when(inner)
        def _():
            z1_inner(s).wait_send()
            z2_copy(s).wait_send()
            z3_copy(s).wait_send()

    def f_start(s, begin):
        a, b, span = blocks(s)
        n = size(s) // 2
        owner = a + zh * (b - a)
        src = fbuf.at[s, pl.ds(0, n)]
        dst = dx_ref.at[pl.ds(pl.multiple_of(span[0] * unit + zb * n, n), n)]
        away = jnp.logical_or(z != r, owner != r)

        @pl.when(away)
        def _():
            copy = send(src, dst, f_send.at[s], f_recv.at[0], c=r, rr=owner)
            copy.start() if begin else copy.wait_send()

        if begin:

            @pl.when(jnp.logical_not(away))
            def _():
                pltpu.make_async_copy(src, dst, f_recv.at[0]).start()

    def stage_a(s):
        a, b, span = blocks(s)
        p = s - len(NEAR)
        if p < 0:
            with jax.named_scope(f"wd{s}"):
                d_arrival(s).wait_recv()
        else:
            with jax.named_scope(f"wy{s}"):
                y_arrival(p).wait_recv()
            e_copy(p).start()
            with jax.named_scope(f"we{s}"):
                e_arrival(p).wait_recv()
        if s == 0:
            w_load.wait()
        if s >= SLOTS:
            z_sent(s - SLOTS)
        slot, n = s % SLOTS, 2 * size(s)
        pbuf[slot, :n] = jnp.zeros((n, kb), jnp.float32)

        @pl.loop(0, nb // kc)
        def _(i):
            cols = pl.ds(pl.multiple_of(i * kc, kc), kc)
            lhs = jnp.concatenate([dyf[rows(a, span), cols], dyf[rows(b, span), cols]], axis=0)
            pbuf[slot, :n] += lax.dot_general(
                lhs, wv[:, cols], (((1,), (1,)), ((), ())), preferred_element_type=jnp.float32
            )

        @pl.when(end)
        def _():
            z1_end(s).start()

        @pl.when(inner)
        def _():
            z1_inner(s).start()

    def stage_b(s):
        n = size(s) // 2

        @pl.when(inner)
        def _():
            z1_end(s).wait_recv()
            pbuf[s % SLOTS, at(2 * (1 - zh), n, 2)] += rb1[s, at(1 - zh, n, 2)]
            z3_copy(s).start()
            z2_copy(s).start()

    def stage_c(s):
        n = size(s) // 2

        @pl.when(end)
        def _():
            z1_inner(s).wait_recv()

        z2_copy(s).wait_recv()
        mine = jnp.where(inner, 2 * zh, 0)
        total = (pbuf[s % SLOTS, at(z, n)] + rb1[s, at(mine, n)]) + rb2[s, :n]
        fbuf[s, :n] = total.astype(fbuf.dtype)
        f_start(s, True)

    def o_copy(j, slot):
        cols = pl.ds(pl.multiple_of(j * nc, nc), nc)
        return pltpu.make_async_copy(obuf.at[slot], dw_ref.at[:, cols], o_sem.at[slot])

    early = [pl.ds(pl.multiple_of(y * 2 * tb, 2 * tb), 2 * tb), rows(2 * (1 - y), (0, LATE)), rows(3 - 2 * y, (0, LATE))]

    def dw_early(lo, hi):
        chunks = nb // nc

        @pl.loop((lo * chunks) // 14, (hi * chunks) // 14)
        def _(j):
            slot = j % 2

            @pl.when(j >= 2)
            def _():
                o_copy(j - 2, slot).wait()

            cols = pl.ds(pl.multiple_of(j * nc, nc), nc)
            terms = [
                lax.dot_general(xf[at], dyf[at, cols], (((0,), (0,)), ((), ())), preferred_element_type=jnp.float32)
                for at in early
            ]
            obuf[slot] = (terms[0] + terms[1]) + terms[2]
            o_copy(j, slot).start()

    late = (8 - LATE) * unit

    def x_late(i):
        src = xf.at[rows((over, over_mate)[i], (LATE, 8 - LATE))]
        return pltpu.make_async_copy(src, xl_ref.at[pl.ds(i * late, late)], l_sem.at[i])

    def dy_late(i):
        src = dyf.at[rows((over, over_mate)[i], (LATE, 8 - LATE))]
        return pltpu.make_async_copy(src, dyl_ref.at[pl.ds(i * late, late)], l_sem.at[2 + i])

    with jax.named_scope("a0"):
        stage_a(0)
    with jax.named_scope("x0"):
        x_point(0)
    with jax.named_scope("a1"):
        stage_a(1)
    with jax.named_scope("y_rest"):
        y_rest()
    with jax.named_scope("a2"):
        stage_a(2)
    with jax.named_scope("a3"):
        stage_a(3)
    with jax.named_scope("b0"):
        stage_b(0)
    with jax.named_scope("x1"):
        x_point(1)
    with jax.named_scope("b1"):
        stage_b(1)
    with jax.named_scope("c0"):
        stage_c(0)
    with jax.named_scope("x2"):
        x_point(2)
    with jax.named_scope("b2"):
        stage_b(2)
    with jax.named_scope("c1"):
        stage_c(1)
    with jax.named_scope("x3"):
        x_point(3)
    with jax.named_scope("a4"):
        stage_a(4)
    with jax.named_scope("b3"):
        stage_b(3)
    with jax.named_scope("c2"):
        stage_c(2)
    with jax.named_scope("x4"):
        x_point(4)
    with jax.named_scope("c3"):
        stage_c(3)
    with jax.named_scope("b4"):
        stage_b(4)
    with jax.named_scope("x5"):
        x_point(5)
    with jax.named_scope("c4"):
        stage_c(4)
    with jax.named_scope("a5"):
        stage_a(5)
    with jax.named_scope("x6"):
        x_point(6)
    with jax.named_scope("b5"):
        stage_b(5)
    with jax.named_scope("c5"):
        stage_c(5)
    with jax.named_scope("x7"):
        x_point(7)
    with jax.named_scope("a6"):
        stage_a(6)
    x_late(0).start()
    x_late(1).start()
    with jax.named_scope("b6"):
        stage_b(6)
    with jax.named_scope("a7"):
        stage_a(7)
    with jax.named_scope("c6"):
        stage_c(6)
    with jax.named_scope("dw0_3"):
        dw_early(0, 3)
    with jax.named_scope("b7"):
        stage_b(7)
    with jax.named_scope("dw3_6"):
        dw_early(3, 6)
    with jax.named_scope("c7"):
        stage_c(7)
    with jax.named_scope("a8"):
        stage_a(8)
    dy_late(0).start()
    dy_late(1).start()
    with jax.named_scope("dw6_10"):
        dw_early(6, 10)
    with jax.named_scope("b8"):
        stage_b(8)
    with jax.named_scope("dw10_14"):
        dw_early(10, 14)
    with jax.named_scope("c8"):
        stage_c(8)

    chunks = nb // nc
    for j in (chunks - 2, chunks - 1):
        o_copy(j, j % 2).wait()
    for p in range(len(NEAR)):
        d_copy(p).wait_send()
    for p in range(len(FAR)):
        y_copy(p).wait_send()
        e_copy(p).wait_send()
    for s in range(STEPS - SLOTS, STEPS):
        z_sent(s)
    for s in range(STEPS):
        f_start(s, False)
    for t in range(4):
        _, go_right, go_left = routes[t]

        @pl.when(go_right)
        def _():
            x_right_copy(t).wait_send()

        @pl.when(go_left)
        def _():
            x_left_copy(t).wait_send()

    @pl.when(direct)
    def _():
        x_out.wait_send()

    @pl.when(detour)
    def _():
        m_out.wait_send()

    @pl.when(relay)
    def _():
        m_pass.wait_send()

    for i in range(2):
        x_late(i).wait()
        dy_late(i).wait()
    pltpu.make_async_copy(dx_ref, dx_ref, f_recv.at[0]).wait()


def solution(mesh):
    rows = P(("data", "r"), "c")

    def local(x, w, dy):
        tb, kb = x.shape
        nb = dy.shape[1]
        pr, late = tb // 4, 2 * tb * (8 - LATE) // 8
        nc = pick(nb, 512)
        any_spec = pl.BlockSpec(memory_space=pl.ANY)
        dma = pltpu.SemaphoreType.DMA
        far, steps = (len(FAR),), (STEPS,)
        dx, dw_early, x_late, dy_late = pl.pallas_call(
            kernel,
            name="linear_backward",
            out_shape=(
                jax.ShapeDtypeStruct((tb, kb), jnp.bfloat16),
                jax.ShapeDtypeStruct((kb, nb), jnp.float32),
                jax.ShapeDtypeStruct((late, kb), jnp.bfloat16),
                jax.ShapeDtypeStruct((late, nb), jnp.bfloat16),
            ),
            in_specs=[any_spec] * 3,
            out_specs=(any_spec,) * 4,
            scratch_shapes=[
                pltpu.VMEM((4 * tb, nb), jnp.bfloat16),
                pltpu.VMEM((kb, nb), jnp.bfloat16),
                pltpu.VMEM((4 * tb, kb), jnp.bfloat16),
                pltpu.VMEM((tb, kb), jnp.bfloat16),
                pltpu.VMEM((SLOTS, 2 * pr, kb), jnp.float32),
                pltpu.VMEM((STEPS, 3 * pr // 2, kb), jnp.float32),
                pltpu.VMEM((STEPS, pr // 2, kb), jnp.float32),
                pltpu.VMEM((STEPS, pr // 2, kb), jnp.bfloat16),
                pltpu.VMEM((2, kb, nc), jnp.float32),
                dma((len(NEAR),)), dma, dma(far), dma(far), dma((len(NEAR),)), dma((len(NEAR),)), dma(far), dma(far),
                dma(steps), dma(steps), dma(steps), dma(steps), dma(steps), dma(steps), dma((1,)),
                dma((1,)), dma((4,)), dma((4,)), dma((4,)), dma((3,)), dma((2,)), dma((4,)),
            ],
            compiler_params=pltpu.CompilerParams(
                collective_id=0, has_side_effects=True, vmem_limit_bytes=67_000_000
            ),
        )(x, w, dy)
        dw_late = lax.dot_general(x_late, dy_late, (((0,), (0,)), ((), ())), preferred_element_type=jnp.float32)
        return dx, dw_early + dw_late

    return jax.shard_map(local, mesh=mesh, in_specs=(rows, P("r", "c"), rows), out_specs=(rows, rows), check_vma=False)
```

```python
import jax
import jax.numpy as jnp
from jax import lax
from jax.experimental import pallas as pl
from jax.experimental.pallas import tpu as pltpu
from jax.sharding import PartitionSpec as P

MESH = pl.DeviceIdType.MESH
NEAR = ((0, 2), (2, 2), (4, 2), (6, 2))
FAR = ((0, 2), (2, 2), (4, 2), (6, 1), (7, 1))
LATE = 4
STEPS = len(NEAR) + len(FAR)
SLOTS = 4


def pick(size, want):
    return want if size % want == 0 else 128


def kernel(
    x_ref, w_ref, dy_ref, dx_ref, dw_ref, xl_ref, dyl_ref,
    dyf, wv, xf, xmid, pbuf, rb1, rb2, fbuf, obuf,
    ld_sem, w_sem, y_send, y_recv, d_send, d_recv, e_send, e_recv,
    z1_send, z1_recv, z2_send, z3_send, z2_recv, f_send, f_recv,
    x_src, x_recv, x_left, x_right, m_sem, o_sem, l_sem,
):
    z, r = lax.axis_index("c"), lax.axis_index("r")
    y, k = r // 2, r % 2
    mate, over, over_mate = 2 * y + 1 - k, 2 * (1 - y) + k, 2 * (1 - y) + 1 - k
    zb, zh = z % 2, z // 2
    z1, z2 = 2 * zh + 1 - zb, 2 * (1 - zh) + zb
    tb, kb = x_ref.shape
    nb = dy_ref.shape[1]
    unit = tb // 8
    kc, nc = pick(nb, 1024), pick(nb, 512)

    def rows(block, span):
        return pl.ds(pl.multiple_of(block * tb + span[0] * unit, unit), span[1] * unit)

    def send(src, dst, ssem, rsem, c=None, rr=None):
        dev = {}
        if c is not None:
            dev["c"] = c
        if rr is not None:
            dev["r"] = rr
        return pltpu.make_async_remote_copy(
            src_ref=src, dst_ref=dst, send_sem=ssem, recv_sem=rsem, device_id=dev, device_id_type=MESH
        )

    def load(p):
        src = dy_ref.at[pl.ds(NEAR[p][0] * unit, NEAR[p][1] * unit)]
        return pltpu.make_async_copy(src, dyf.at[rows(r, NEAR[p])], ld_sem.at[p])

    w_load = pltpu.make_async_copy(w_ref, wv, w_sem)
    for p in range(len(NEAR)):
        load(p).start()
    w_load.start()

    barrier = pltpu.get_barrier_semaphore()
    for i in range(1, 16):
        peer = {"c": (z + i // 4) % 4, "r": (r + i % 4) % 4}
        pl.semaphore_signal(barrier, inc=1, device_id=peer, device_id_type=MESH)
    pl.semaphore_wait(barrier, 15)

    def xrows(t):
        return pl.ds(pl.multiple_of(t * tb, tb), tb)

    detour = jnp.logical_and(k == 1, y != zh)
    relay = jnp.logical_and(k == 1, y == zh)
    direct = jnp.logical_and(jnp.logical_not(detour), r != z)
    x_own = pltpu.make_async_copy(x_ref, xf.at[xrows(r)], x_recv.at[r])
    x_out = send(x_ref, xf.at[xrows(r)], x_src.at[0], x_recv.at[r], c=z, rr=z)
    m_out = send(x_ref, xmid, m_sem.at[0], m_sem.at[1], c=z2)
    m_pass = send(xmid, xf.at[xrows(r)], m_sem.at[2], x_recv.at[r], c=z, rr=z2)

    @pl.when(r == z)
    def _():
        x_own.start()

    @pl.when(direct)
    def _():
        x_out.start()

    @pl.when(detour)
    def _():
        m_out.start()

    def y_copy(p):
        return send(dyf.at[rows(r, FAR[p])], dyf.at[rows(r, FAR[p])], y_send.at[p], y_recv.at[p], rr=over)

    def d_copy(p):
        return send(dyf.at[rows(r, NEAR[p])], dyf.at[rows(r, NEAR[p])], d_send.at[p], d_recv.at[p], rr=mate)

    def e_copy(p):
        return send(dyf.at[rows(over, FAR[p])], dyf.at[rows(over, FAR[p])], e_send.at[p], e_recv.at[p], rr=mate)

    def y_arrival(p):
        return send(dyf.at[rows(over, FAR[p])], dyf.at[rows(over, FAR[p])], y_send.at[p], y_recv.at[p], rr=over)

    def d_arrival(p):
        return send(dyf.at[rows(mate, NEAR[p])], dyf.at[rows(mate, NEAR[p])], d_send.at[p], d_recv.at[p], rr=mate)

    def e_arrival(p):
        at = rows(over_mate, FAR[p])
        return send(dyf.at[at], dyf.at[at], e_send.at[p], e_recv.at[p], rr=mate)

    for p in range(len(NEAR)):
        load(p).wait()
        if p == 0:
            y_copy(0).start()
        d_copy(p).start()

    def y_rest():
        @pl.when(relay)
        def _():
            m_out.wait_recv()
            m_pass.start()

        for p in range(1, len(FAR)):
            y_copy(p).start()

    def x_route(t):
        near = y == t // 2
        head = jnp.where(jnp.logical_or(near, t % 2 == 0), r, (r + 2) % 4)
        hops = jnp.where(z >= head, z - head, head - z)
        turn = jnp.where(near, t % 2, 2 + t % 2)
        go_right = jnp.logical_and(z >= head, z < 3)
        go_left = jnp.logical_and(z <= head, z > 0)
        return turn + hops, go_right, go_left

    routes = [x_route(t) for t in range(4)]

    def x_right_copy(t):
        return send(xf.at[xrows(t)], xf.at[xrows(t)], x_right.at[t], x_recv.at[t], c=z + 1)

    def x_left_copy(t):
        return send(xf.at[xrows(t)], xf.at[xrows(t)], x_left.at[t], x_recv.at[t], c=z - 1)

    def x_point(j):
        for t in range(4):
            when, go_right, go_left = routes[t]
            live = when == j

            @pl.when(live)
            def _():
                pltpu.make_async_copy(x_ref, xf.at[xrows(t)], x_recv.at[t]).wait()

            @pl.when(jnp.logical_and(live, go_right))
            def _():
                x_right_copy(t).start()

            @pl.when(jnp.logical_and(live, go_left))
            def _():
                x_left_copy(t).start()

    def blocks(s):
        return (r, mate, NEAR[s]) if s < len(NEAR) else (over, over_mate, FAR[s - len(NEAR)])

    def size(s):
        return blocks(s)[2][1] * unit

    inner = jnp.logical_or(z == 1, z == 2)
    end = jnp.logical_not(inner)
    far_end = 3 * (1 - zh)

    def at(first, n, count=1):
        return pl.ds(pl.multiple_of(first * n, n), count * n)

    def z1_end(s):
        n = size(s) // 2
        src = pbuf.at[s % SLOTS, at(1 - zh, n, 3)]
        return send(src, rb1.at[s, pl.ds(0, 3 * n)], z1_send.at[s], z1_recv.at[s], c=z1)

    def z1_inner(s):
        n = size(s) // 2
        src = pbuf.at[s % SLOTS, at(3 * zh, n)]
        return send(src, rb1.at[s, pl.ds(0, n)], z1_send.at[s], z1_recv.at[s], c=z1)

    def z2_copy(s):
        n = size(s) // 2
        return send(pbuf.at[s % SLOTS, at(3 - z, n)], rb2.at[s, pl.ds(0, n)], z2_send.at[s], z2_recv.at[s], c=3 - z)

    def z3_copy(s):
        n = size(s) // 2
        src = pbuf.at[s % SLOTS, at(far_end, n)]
        return send(src, rb2.at[s, pl.ds(0, n)], z3_send.at[s], z2_recv.at[s], c=far_end)

    def z_sent(s):
        @pl.when(end)
        def _():
            z1_end(s).wait_send()

        @pl.when(inner)
        def _():
            z1_inner(s).wait_send()
            z2_copy(s).wait_send()
            z3_copy(s).wait_send()

    def f_start(s, begin):
        a, b, span = blocks(s)
        n = size(s) // 2
        owner = a + zh * (b - a)
        src = fbuf.at[s, pl.ds(0, n)]
        dst = dx_ref.at[pl.ds(pl.multiple_of(span[0] * unit + zb * n, n), n)]
        away = jnp.logical_or(z != r, owner != r)

        @pl.when(away)
        def _():
            copy = send(src, dst, f_send.at[s], f_recv.at[0], c=r, rr=owner)
            copy.start() if begin else copy.wait_send()

        if begin:

            @pl.when(jnp.logical_not(away))
            def _():
                pltpu.make_async_copy(src, dst, f_recv.at[0]).start()

    def stage_a(s):
        a, b, span = blocks(s)
        p = s - len(NEAR)
        if p < 0:
            with jax.named_scope(f"wd{s}"):
                d_arrival(s).wait_recv()
        else:
            with jax.named_scope(f"wy{s}"):
                y_arrival(p).wait_recv()
            e_copy(p).start()
            with jax.named_scope(f"we{s}"):
                e_arrival(p).wait_recv()
        if s == 0:
            w_load.wait()
        if s >= SLOTS:
            z_sent(s - SLOTS)
        slot, n = s % SLOTS, 2 * size(s)
        pbuf[slot, :n] = jnp.zeros((n, kb), jnp.float32)

        @pl.loop(0, nb // kc)
        def _(i):
            cols = pl.ds(pl.multiple_of(i * kc, kc), kc)
            lhs = jnp.concatenate([dyf[rows(a, span), cols], dyf[rows(b, span), cols]], axis=0)
            pbuf[slot, :n] += lax.dot_general(
                lhs, wv[:, cols], (((1,), (1,)), ((), ())), preferred_element_type=jnp.float32
            )

        @pl.when(end)
        def _():
            z1_end(s).start()

        @pl.when(inner)
        def _():
            z1_inner(s).start()

    def stage_b(s):
        n = size(s) // 2

        @pl.when(inner)
        def _():
            z1_end(s).wait_recv()
            pbuf[s % SLOTS, at(2 * (1 - zh), n, 2)] += rb1[s, at(1 - zh, n, 2)]
            z3_copy(s).start()
            z2_copy(s).start()

    def stage_c(s):
        n = size(s) // 2

        @pl.when(end)
        def _():
            z1_inner(s).wait_recv()

        z2_copy(s).wait_recv()
        mine = jnp.where(inner, 2 * zh, 0)
        total = (pbuf[s % SLOTS, at(z, n)] + rb1[s, at(mine, n)]) + rb2[s, :n]
        fbuf[s, :n] = total.astype(fbuf.dtype)
        f_start(s, True)

    def o_copy(j, slot):
        cols = pl.ds(pl.multiple_of(j * nc, nc), nc)
        return pltpu.make_async_copy(obuf.at[slot], dw_ref.at[:, cols], o_sem.at[slot])

    early = [pl.ds(pl.multiple_of(y * 2 * tb, 2 * tb), 2 * tb), rows(2 * (1 - y), (0, LATE)), rows(3 - 2 * y, (0, LATE))]

    def dw_early(lo, hi):
        chunks = nb // nc

        @pl.loop((lo * chunks) // 14, (hi * chunks) // 14)
        def _(j):
            slot = j % 2

            @pl.when(j >= 2)
            def _():
                o_copy(j - 2, slot).wait()

            cols = pl.ds(pl.multiple_of(j * nc, nc), nc)
            terms = [
                lax.dot_general(xf[at], dyf[at, cols], (((0,), (0,)), ((), ())), preferred_element_type=jnp.float32)
                for at in early
            ]
            obuf[slot] = (terms[0] + terms[1]) + terms[2]
            o_copy(j, slot).start()

    late = (8 - LATE) * unit

    def x_late(i):
        src = xf.at[rows((over, over_mate)[i], (LATE, 8 - LATE))]
        return pltpu.make_async_copy(src, xl_ref.at[pl.ds(i * late, late)], l_sem.at[i])

    def dy_late(i):
        src = dyf.at[rows((over, over_mate)[i], (LATE, 8 - LATE))]
        return pltpu.make_async_copy(src, dyl_ref.at[pl.ds(i * late, late)], l_sem.at[2 + i])

    with jax.named_scope("a0"):
        stage_a(0)
    with jax.named_scope("x0"):
        x_point(0)
    with jax.named_scope("a1"):
        stage_a(1)
    with jax.named_scope("y_rest"):
        y_rest()
    with jax.named_scope("a2"):
        stage_a(2)
    with jax.named_scope("a3"):
        stage_a(3)
    with jax.named_scope("b0"):
        stage_b(0)
    with jax.named_scope("b1"):
        stage_b(1)
    with jax.named_scope("c0"):
        stage_c(0)
    with jax.named_scope("x1"):
        x_point(1)
    with jax.named_scope("b2"):
        stage_b(2)
    with jax.named_scope("c1"):
        stage_c(1)
    with jax.named_scope("a4"):
        stage_a(4)
    with jax.named_scope("b3"):
        stage_b(3)
    with jax.named_scope("c2"):
        stage_c(2)
    with jax.named_scope("x2"):
        x_point(2)
    with jax.named_scope("c3"):
        stage_c(3)
    with jax.named_scope("b4"):
        stage_b(4)
    with jax.named_scope("x3"):
        x_point(3)
    with jax.named_scope("c4"):
        stage_c(4)
    with jax.named_scope("a5"):
        stage_a(5)
    with jax.named_scope("b5"):
        stage_b(5)
    with jax.named_scope("x4"):
        x_point(4)
    with jax.named_scope("c5"):
        stage_c(5)
    with jax.named_scope("a6"):
        stage_a(6)
    with jax.named_scope("x5"):
        x_point(5)
    with jax.named_scope("b6"):
        stage_b(6)
    with jax.named_scope("a7"):
        stage_a(7)
    with jax.named_scope("x6"):
        x_point(6)
    x_late(0).start()
    x_late(1).start()
    with jax.named_scope("c6"):
        stage_c(6)
    with jax.named_scope("dw0_3"):
        dw_early(0, 3)
    with jax.named_scope("b7"):
        stage_b(7)
    with jax.named_scope("dw3_6"):
        dw_early(3, 6)
    with jax.named_scope("c7"):
        stage_c(7)
    with jax.named_scope("a8"):
        stage_a(8)
    dy_late(0).start()
    dy_late(1).start()
    with jax.named_scope("dw6_10"):
        dw_early(6, 10)
    with jax.named_scope("b8"):
        stage_b(8)
    with jax.named_scope("dw10_14"):
        dw_early(10, 14)
    with jax.named_scope("c8"):
        stage_c(8)

    chunks = nb // nc
    for j in (chunks - 2, chunks - 1):
        o_copy(j, j % 2).wait()
    for p in range(len(NEAR)):
        d_copy(p).wait_send()
    for p in range(len(FAR)):
        y_copy(p).wait_send()
        e_copy(p).wait_send()
    for s in range(STEPS - SLOTS, STEPS):
        z_sent(s)
    for s in range(STEPS):
        f_start(s, False)
    for t in range(4):
        _, go_right, go_left = routes[t]

        @pl.when(go_right)
        def _():
            x_right_copy(t).wait_send()

        @pl.when(go_left)
        def _():
            x_left_copy(t).wait_send()

    @pl.when(direct)
    def _():
        x_out.wait_send()

    @pl.when(detour)
    def _():
        m_out.wait_send()

    @pl.when(relay)
    def _():
        m_pass.wait_send()

    for i in range(2):
        x_late(i).wait()
        dy_late(i).wait()
    pltpu.make_async_copy(dx_ref, dx_ref, f_recv.at[0]).wait()


def solution(mesh):
    rows = P(("data", "r"), "c")

    def local(x, w, dy):
        tb, kb = x.shape
        nb = dy.shape[1]
        pr, late = tb // 4, 2 * tb * (8 - LATE) // 8
        nc = pick(nb, 512)
        any_spec = pl.BlockSpec(memory_space=pl.ANY)
        dma = pltpu.SemaphoreType.DMA
        far, steps = (len(FAR),), (STEPS,)
        dx, dw_early, x_late, dy_late = pl.pallas_call(
            kernel,
            name="linear_backward",
            out_shape=(
                jax.ShapeDtypeStruct((tb, kb), jnp.bfloat16),
                jax.ShapeDtypeStruct((kb, nb), jnp.float32),
                jax.ShapeDtypeStruct((late, kb), jnp.bfloat16),
                jax.ShapeDtypeStruct((late, nb), jnp.bfloat16),
            ),
            in_specs=[any_spec] * 3,
            out_specs=(any_spec,) * 4,
            scratch_shapes=[
                pltpu.VMEM((4 * tb, nb), jnp.bfloat16),
                pltpu.VMEM((kb, nb), jnp.bfloat16),
                pltpu.VMEM((4 * tb, kb), jnp.bfloat16),
                pltpu.VMEM((tb, kb), jnp.bfloat16),
                pltpu.VMEM((SLOTS, 2 * pr, kb), jnp.float32),
                pltpu.VMEM((STEPS, 3 * pr // 2, kb), jnp.float32),
                pltpu.VMEM((STEPS, pr // 2, kb), jnp.float32),
                pltpu.VMEM((STEPS, pr // 2, kb), jnp.bfloat16),
                pltpu.VMEM((2, kb, nc), jnp.float32),
                dma((len(NEAR),)), dma, dma(far), dma(far), dma((len(NEAR),)), dma((len(NEAR),)), dma(far), dma(far),
                dma(steps), dma(steps), dma(steps), dma(steps), dma(steps), dma(steps), dma((1,)),
                dma((1,)), dma((4,)), dma((4,)), dma((4,)), dma((3,)), dma((2,)), dma((4,)),
            ],
            compiler_params=pltpu.CompilerParams(
                collective_id=0, has_side_effects=True, vmem_limit_bytes=67_000_000
            ),
        )(x, w, dy)
        dw_late = lax.dot_general(x_late, dy_late, (((0,), (0,)), ((), ())), preferred_element_type=jnp.float32)
        return dx, dw_early + dw_late

    return jax.shard_map(local, mesh=mesh, in_specs=(rows, P("r", "c"), rows), out_specs=(rows, rows), check_vma=False)
```

```python
import jax
import jax.numpy as jnp
from jax import lax
from jax.experimental import pallas as pl
from jax.experimental.pallas import tpu as pltpu
from jax.sharding import PartitionSpec as P

MESH = pl.DeviceIdType.MESH
NEAR = ((0, 2), (2, 2), (4, 2), (6, 2))
FAR = ((0, 2), (2, 2), (4, 2), (6, 1), (7, 1))
LATE = 4
STEPS = len(NEAR) + len(FAR)
SLOTS = 4


def pick(size, want):
    return want if size % want == 0 else 128


def kernel(
    x_ref, w_ref, dy_ref, dx_ref, dw_ref, xl_ref, dyl_ref,
    dyf, wv, xf, xmid, pbuf, rb1, rb2, fbuf, obuf,
    ld_sem, w_sem, y_send, y_recv, d_send, d_recv, e_send, e_recv,
    z1_send, z1_recv, z2_send, z3_send, z2_recv, f_send, f_recv,
    x_src, x_recv, x_left, x_right, m_sem, o_sem, l_sem,
):
    z, r = lax.axis_index("c"), lax.axis_index("r")
    y, k = r // 2, r % 2
    mate, over, over_mate = 2 * y + 1 - k, 2 * (1 - y) + k, 2 * (1 - y) + 1 - k
    zb, zh = z % 2, z // 2
    z1, z2 = 2 * zh + 1 - zb, 2 * (1 - zh) + zb
    tb, kb = x_ref.shape
    nb = dy_ref.shape[1]
    unit = tb // 8
    kc, nc = pick(nb, 1024), pick(nb, 512)

    def rows(block, span):
        return pl.ds(pl.multiple_of(block * tb + span[0] * unit, unit), span[1] * unit)

    def send(src, dst, ssem, rsem, c=None, rr=None):
        dev = {}
        if c is not None:
            dev["c"] = c
        if rr is not None:
            dev["r"] = rr
        return pltpu.make_async_remote_copy(
            src_ref=src, dst_ref=dst, send_sem=ssem, recv_sem=rsem, device_id=dev, device_id_type=MESH
        )

    def load(p):
        src = dy_ref.at[pl.ds(NEAR[p][0] * unit, NEAR[p][1] * unit)]
        return pltpu.make_async_copy(src, dyf.at[rows(r, NEAR[p])], ld_sem.at[p])

    w_load = pltpu.make_async_copy(w_ref, wv, w_sem)
    for p in range(len(NEAR)):
        load(p).start()
    w_load.start()

    barrier = pltpu.get_barrier_semaphore()
    for i in range(1, 16):
        peer = {"c": (z + i // 4) % 4, "r": (r + i % 4) % 4}
        pl.semaphore_signal(barrier, inc=1, device_id=peer, device_id_type=MESH)
    pl.semaphore_wait(barrier, 15)

    def xrows(t):
        return pl.ds(pl.multiple_of(t * tb, tb), tb)

    detour = jnp.logical_and(k == 1, y != zh)
    relay = jnp.logical_and(k == 1, y == zh)
    direct = jnp.logical_and(jnp.logical_not(detour), r != z)
    x_own = pltpu.make_async_copy(x_ref, xf.at[xrows(r)], x_recv.at[r])
    x_out = send(x_ref, xf.at[xrows(r)], x_src.at[0], x_recv.at[r], c=z, rr=z)
    m_out = send(x_ref, xmid, m_sem.at[0], m_sem.at[1], c=z2)
    m_pass = send(xmid, xf.at[xrows(r)], m_sem.at[2], x_recv.at[r], c=z, rr=z2)

    @pl.when(r == z)
    def _():
        x_own.start()

    @pl.when(direct)
    def _():
        x_out.start()

    @pl.when(detour)
    def _():
        m_out.start()

    def y_copy(p):
        return send(dyf.at[rows(r, FAR[p])], dyf.at[rows(r, FAR[p])], y_send.at[p], y_recv.at[p], rr=over)

    def d_copy(p):
        return send(dyf.at[rows(r, NEAR[p])], dyf.at[rows(r, NEAR[p])], d_send.at[p], d_recv.at[p], rr=mate)

    def e_copy(p):
        return send(dyf.at[rows(over, FAR[p])], dyf.at[rows(over, FAR[p])], e_send.at[p], e_recv.at[p], rr=mate)

    def y_arrival(p):
        return send(dyf.at[rows(over, FAR[p])], dyf.at[rows(over, FAR[p])], y_send.at[p], y_recv.at[p], rr=over)

    def d_arrival(p):
        return send(dyf.at[rows(mate, NEAR[p])], dyf.at[rows(mate, NEAR[p])], d_send.at[p], d_recv.at[p], rr=mate)

    def e_arrival(p):
        at = rows(over_mate, FAR[p])
        return send(dyf.at[at], dyf.at[at], e_send.at[p], e_recv.at[p], rr=mate)

    for p in range(len(NEAR)):
        load(p).wait()
        if p == 0:
            y_copy(0).start()
        d_copy(p).start()

    def y_rest():
        @pl.when(relay)
        def _():
            m_out.wait_recv()
            m_pass.start()

        for p in range(1, len(FAR)):
            y_copy(p).start()

    def x_route(t):
        near = y == t // 2
        head = jnp.where(jnp.logical_or(near, t % 2 == 0), r, (r + 2) % 4)
        hops = jnp.where(z >= head, z - head, head - z)
        turn = jnp.where(near, t % 2, 2 + t % 2)
        go_right = jnp.logical_and(z >= head, z < 3)
        go_left = jnp.logical_and(z <= head, z > 0)
        return turn + hops, go_right, go_left

    routes = [x_route(t) for t in range(4)]

    def x_right_copy(t):
        return send(xf.at[xrows(t)], xf.at[xrows(t)], x_right.at[t], x_recv.at[t], c=z + 1)

    def x_left_copy(t):
        return send(xf.at[xrows(t)], xf.at[xrows(t)], x_left.at[t], x_recv.at[t], c=z - 1)

    def x_point(j):
        for t in range(4):
            when, go_right, go_left = routes[t]
            live = when == j

            @pl.when(live)
            def _():
                pltpu.make_async_copy(x_ref, xf.at[xrows(t)], x_recv.at[t]).wait()

            @pl.when(jnp.logical_and(live, go_right))
            def _():
                x_right_copy(t).start()

            @pl.when(jnp.logical_and(live, go_left))
            def _():
                x_left_copy(t).start()

    def blocks(s):
        return (r, mate, NEAR[s]) if s < len(NEAR) else (over, over_mate, FAR[s - len(NEAR)])

    def size(s):
        return blocks(s)[2][1] * unit

    inner = jnp.logical_or(z == 1, z == 2)
    end = jnp.logical_not(inner)
    far_end = 3 * (1 - zh)

    def at(first, n, count=1):
        return pl.ds(pl.multiple_of(first * n, n), count * n)

    def z1_end(s):
        n = size(s) // 2
        src = pbuf.at[s % SLOTS, at(1 - zh, n, 3)]
        return send(src, rb1.at[s, pl.ds(0, 3 * n)], z1_send.at[s], z1_recv.at[s], c=z1)

    def z1_inner(s):
        n = size(s) // 2
        src = pbuf.at[s % SLOTS, at(3 * zh, n)]
        return send(src, rb1.at[s, pl.ds(0, n)], z1_send.at[s], z1_recv.at[s], c=z1)

    def z2_copy(s):
        n = size(s) // 2
        return send(pbuf.at[s % SLOTS, at(3 - z, n)], rb2.at[s, pl.ds(0, n)], z2_send.at[s], z2_recv.at[s], c=3 - z)

    def z3_copy(s):
        n = size(s) // 2
        src = pbuf.at[s % SLOTS, at(far_end, n)]
        return send(src, rb2.at[s, pl.ds(0, n)], z3_send.at[s], z2_recv.at[s], c=far_end)

    def z_sent(s):
        @pl.when(end)
        def _():
            z1_end(s).wait_send()

        @pl.when(inner)
        def _():
            z1_inner(s).wait_send()
            z2_copy(s).wait_send()
            z3_copy(s).wait_send()

    def f_start(s, begin):
        a, b, span = blocks(s)
        n = size(s) // 2
        owner = a + zh * (b - a)
        src = fbuf.at[s, pl.ds(0, n)]
        dst = dx_ref.at[pl.ds(pl.multiple_of(span[0] * unit + zb * n, n), n)]
        away = jnp.logical_or(z != r, owner != r)

        @pl.when(away)
        def _():
            copy = send(src, dst, f_send.at[s], f_recv.at[0], c=r, rr=owner)
            copy.start() if begin else copy.wait_send()

        if begin:

            @pl.when(jnp.logical_not(away))
            def _():
                pltpu.make_async_copy(src, dst, f_recv.at[0]).start()

    def stage_a(s):
        a, b, span = blocks(s)
        p = s - len(NEAR)
        if p < 0:
            with jax.named_scope(f"wd{s}"):
                d_arrival(s).wait_recv()
        else:
            with jax.named_scope(f"wy{s}"):
                y_arrival(p).wait_recv()
            e_copy(p).start()
            with jax.named_scope(f"we{s}"):
                e_arrival(p).wait_recv()
        if s == 0:
            w_load.wait()
        if s >= SLOTS:
            z_sent(s - SLOTS)
        slot, n = s % SLOTS, 2 * size(s)
        pbuf[slot, :n] = jnp.zeros((n, kb), jnp.float32)

        @pl.loop(0, nb // kc)
        def _(i):
            cols = pl.ds(pl.multiple_of(i * kc, kc), kc)
            lhs = jnp.concatenate([dyf[rows(a, span), cols], dyf[rows(b, span), cols]], axis=0)
            pbuf[slot, :n] += lax.dot_general(
                lhs, wv[:, cols], (((1,), (1,)), ((), ())), preferred_element_type=jnp.float32
            )

        @pl.when(end)
        def _():
            z1_end(s).start()

        @pl.when(inner)
        def _():
            z1_inner(s).start()

    def stage_b(s):
        n = size(s) // 2

        @pl.when(inner)
        def _():
            z1_end(s).wait_recv()
            pbuf[s % SLOTS, at(2 * (1 - zh), n, 2)] += rb1[s, at(1 - zh, n, 2)]
            z3_copy(s).start()
            z2_copy(s).start()

    def stage_c(s):
        n = size(s) // 2

        @pl.when(end)
        def _():
            z1_inner(s).wait_recv()

        z2_copy(s).wait_recv()
        mine = jnp.where(inner, 2 * zh, 0)
        total = (pbuf[s % SLOTS, at(z, n)] + rb1[s, at(mine, n)]) + rb2[s, :n]
        fbuf[s, :n] = total.astype(fbuf.dtype)
        f_start(s, True)

    def o_copy(j, slot):
        cols = pl.ds(pl.multiple_of(j * nc, nc), nc)
        return pltpu.make_async_copy(obuf.at[slot], dw_ref.at[:, cols], o_sem.at[slot])

    early = [pl.ds(pl.multiple_of(y * 2 * tb, 2 * tb), 2 * tb), rows(2 * (1 - y), (0, LATE)), rows(3 - 2 * y, (0, LATE))]

    def dw_early(lo, hi):
        chunks = nb // nc

        @pl.loop((lo * chunks) // 14, (hi * chunks) // 14)
        def _(j):
            slot = j % 2

            @pl.when(j >= 2)
            def _():
                o_copy(j - 2, slot).wait()

            cols = pl.ds(pl.multiple_of(j * nc, nc), nc)
            terms = [
                lax.dot_general(xf[at], dyf[at, cols], (((0,), (0,)), ((), ())), preferred_element_type=jnp.float32)
                for at in early
            ]
            obuf[slot] = (terms[0] + terms[1]) + terms[2]
            o_copy(j, slot).start()

    late = (8 - LATE) * unit

    def x_late(i):
        src = xf.at[rows((over, over_mate)[i], (LATE, 8 - LATE))]
        return pltpu.make_async_copy(src, xl_ref.at[pl.ds(i * late, late)], l_sem.at[i])

    def dy_late(i):
        src = dyf.at[rows((over, over_mate)[i], (LATE, 8 - LATE))]
        return pltpu.make_async_copy(src, dyl_ref.at[pl.ds(i * late, late)], l_sem.at[2 + i])

    with jax.named_scope("a0"):
        stage_a(0)
    with jax.named_scope("x0"):
        x_point(0)
    with jax.named_scope("a1"):
        stage_a(1)
    with jax.named_scope("y_rest"):
        y_rest()
    with jax.named_scope("a2"):
        stage_a(2)
    with jax.named_scope("a3"):
        stage_a(3)
    with jax.named_scope("b0"):
        stage_b(0)
    with jax.named_scope("b1"):
        stage_b(1)
    with jax.named_scope("c0"):
        stage_c(0)
    with jax.named_scope("x1"):
        x_point(1)
    with jax.named_scope("b2"):
        stage_b(2)
    with jax.named_scope("c1"):
        stage_c(1)
    with jax.named_scope("a4"):
        stage_a(4)
    with jax.named_scope("b3"):
        stage_b(3)
    with jax.named_scope("c2"):
        stage_c(2)
    with jax.named_scope("x2"):
        x_point(2)
    with jax.named_scope("c3"):
        stage_c(3)
    with jax.named_scope("b4"):
        stage_b(4)
    with jax.named_scope("c4"):
        stage_c(4)
    with jax.named_scope("a5"):
        stage_a(5)
    with jax.named_scope("x3"):
        x_point(3)
    with jax.named_scope("b5"):
        stage_b(5)
    with jax.named_scope("c5"):
        stage_c(5)
    with jax.named_scope("x4"):
        x_point(4)
    with jax.named_scope("a6"):
        stage_a(6)
    with jax.named_scope("x5"):
        x_point(5)
    with jax.named_scope("b6"):
        stage_b(6)
    with jax.named_scope("a7"):
        stage_a(7)
    with jax.named_scope("c6"):
        stage_c(6)
    with jax.named_scope("b7"):
        stage_b(7)
    with jax.named_scope("a8"):
        stage_a(8)
    dy_late(0).start()
    dy_late(1).start()
    with jax.named_scope("x6"):
        x_point(6)
    x_late(0).start()
    x_late(1).start()
    with jax.named_scope("dw0_5"):
        dw_early(0, 5)
    with jax.named_scope("c7"):
        stage_c(7)
    with jax.named_scope("b8"):
        stage_b(8)
    with jax.named_scope("dw5_10"):
        dw_early(5, 10)
    with jax.named_scope("c8"):
        stage_c(8)
    with jax.named_scope("dw10_14"):
        dw_early(10, 14)

    chunks = nb // nc
    for j in (chunks - 2, chunks - 1):
        o_copy(j, j % 2).wait()
    for p in range(len(NEAR)):
        d_copy(p).wait_send()
    for p in range(len(FAR)):
        y_copy(p).wait_send()
        e_copy(p).wait_send()
    for s in range(STEPS - SLOTS, STEPS):
        z_sent(s)
    for s in range(STEPS):
        f_start(s, False)
    for t in range(4):
        _, go_right, go_left = routes[t]

        @pl.when(go_right)
        def _():
            x_right_copy(t).wait_send()

        @pl.when(go_left)
        def _():
            x_left_copy(t).wait_send()

    @pl.when(direct)
    def _():
        x_out.wait_send()

    @pl.when(detour)
    def _():
        m_out.wait_send()

    @pl.when(relay)
    def _():
        m_pass.wait_send()

    for i in range(2):
        x_late(i).wait()
        dy_late(i).wait()
    pltpu.make_async_copy(dx_ref, dx_ref, f_recv.at[0]).wait()


def solution(mesh):
    rows = P(("data", "r"), "c")

    def local(x, w, dy):
        tb, kb = x.shape
        nb = dy.shape[1]
        pr, late = tb // 4, 2 * tb * (8 - LATE) // 8
        nc = pick(nb, 512)
        any_spec = pl.BlockSpec(memory_space=pl.ANY)
        dma = pltpu.SemaphoreType.DMA
        far, steps = (len(FAR),), (STEPS,)
        dx, dw_early, x_late, dy_late = pl.pallas_call(
            kernel,
            name="linear_backward",
            out_shape=(
                jax.ShapeDtypeStruct((tb, kb), jnp.bfloat16),
                jax.ShapeDtypeStruct((kb, nb), jnp.float32),
                jax.ShapeDtypeStruct((late, kb), jnp.bfloat16),
                jax.ShapeDtypeStruct((late, nb), jnp.bfloat16),
            ),
            in_specs=[any_spec] * 3,
            out_specs=(any_spec,) * 4,
            scratch_shapes=[
                pltpu.VMEM((4 * tb, nb), jnp.bfloat16),
                pltpu.VMEM((kb, nb), jnp.bfloat16),
                pltpu.VMEM((4 * tb, kb), jnp.bfloat16),
                pltpu.VMEM((tb, kb), jnp.bfloat16),
                pltpu.VMEM((SLOTS, 2 * pr, kb), jnp.float32),
                pltpu.VMEM((STEPS, 3 * pr // 2, kb), jnp.float32),
                pltpu.VMEM((STEPS, pr // 2, kb), jnp.float32),
                pltpu.VMEM((STEPS, pr // 2, kb), jnp.bfloat16),
                pltpu.VMEM((2, kb, nc), jnp.float32),
                dma((len(NEAR),)), dma, dma(far), dma(far), dma((len(NEAR),)), dma((len(NEAR),)), dma(far), dma(far),
                dma(steps), dma(steps), dma(steps), dma(steps), dma(steps), dma(steps), dma((1,)),
                dma((1,)), dma((4,)), dma((4,)), dma((4,)), dma((3,)), dma((2,)), dma((4,)),
            ],
            compiler_params=pltpu.CompilerParams(
                collective_id=0, has_side_effects=True, vmem_limit_bytes=67_000_000
            ),
        )(x, w, dy)
        dw_late = lax.dot_general(x_late, dy_late, (((0,), (0,)), ((), ())), preferred_element_type=jnp.float32)
        return dx, dw_early + dw_late

    return jax.shard_map(local, mesh=mesh, in_specs=(rows, P("r", "c"), rows), out_specs=(rows, rows), check_vma=False)
```

```python
import jax
import jax.numpy as jnp
from jax import lax
from jax.experimental import pallas as pl
from jax.experimental.pallas import tpu as pltpu
from jax.sharding import PartitionSpec as P

MESH = pl.DeviceIdType.MESH
NEAR = ((0, 2), (2, 2), (4, 2), (6, 2))
FAR = ((0, 2), (2, 2), (4, 2), (6, 1), (7, 1))
LATE = 4
STEPS = len(NEAR) + len(FAR)
SLOTS = 4


def pick(size, want):
    return want if size % want == 0 else 128


def kernel(
    x_ref, w_ref, dy_ref, dx_ref, dw_ref, xl_ref, dyl_ref,
    dyf, wv, xf, xmid, pbuf, rb1, rb2, fbuf, obuf,
    ld_sem, w_sem, y_send, y_recv, d_send, d_recv, e_send, e_recv,
    z1_send, z1_recv, z2_send, z3_send, z2_recv, f_send, f_recv,
    x_src, x_recv, x_left, x_right, m_sem, o_sem, l_sem,
):
    z, r = lax.axis_index("c"), lax.axis_index("r")
    y, k = r // 2, r % 2
    mate, over, over_mate = 2 * y + 1 - k, 2 * (1 - y) + k, 2 * (1 - y) + 1 - k
    zb, zh = z % 2, z // 2
    z1, z2 = 2 * zh + 1 - zb, 2 * (1 - zh) + zb
    tb, kb = x_ref.shape
    nb = dy_ref.shape[1]
    unit = tb // 8
    kc, nc = pick(nb, 1024), pick(nb, 512)

    def rows(block, span):
        return pl.ds(pl.multiple_of(block * tb + span[0] * unit, unit), span[1] * unit)

    def send(src, dst, ssem, rsem, c=None, rr=None):
        dev = {}
        if c is not None:
            dev["c"] = c
        if rr is not None:
            dev["r"] = rr
        return pltpu.make_async_remote_copy(
            src_ref=src, dst_ref=dst, send_sem=ssem, recv_sem=rsem, device_id=dev, device_id_type=MESH
        )

    def load(p):
        src = dy_ref.at[pl.ds(NEAR[p][0] * unit, NEAR[p][1] * unit)]
        return pltpu.make_async_copy(src, dyf.at[rows(r, NEAR[p])], ld_sem.at[p])

    w_load = pltpu.make_async_copy(w_ref, wv, w_sem)
    for p in range(len(NEAR)):
        load(p).start()
    w_load.start()

    barrier = pltpu.get_barrier_semaphore()
    for i in range(1, 16):
        peer = {"c": (z + i // 4) % 4, "r": (r + i % 4) % 4}
        pl.semaphore_signal(barrier, inc=1, device_id=peer, device_id_type=MESH)
    pl.semaphore_wait(barrier, 15)

    def xrows(t):
        return pl.ds(pl.multiple_of(t * tb, tb), tb)

    detour = jnp.logical_and(k == 1, y != zh)
    relay = jnp.logical_and(k == 1, y == zh)
    direct = jnp.logical_and(jnp.logical_not(detour), r != z)
    x_own = pltpu.make_async_copy(x_ref, xf.at[xrows(r)], x_recv.at[r])
    x_out = send(x_ref, xf.at[xrows(r)], x_src.at[0], x_recv.at[r], c=z, rr=z)
    m_out = send(x_ref, xmid, m_sem.at[0], m_sem.at[1], c=z2)
    m_pass = send(xmid, xf.at[xrows(r)], m_sem.at[2], x_recv.at[r], c=z, rr=z2)

    @pl.when(r == z)
    def _():
        x_own.start()

    @pl.when(direct)
    def _():
        x_out.start()

    @pl.when(detour)
    def _():
        m_out.start()

    def y_copy(p):
        return send(dyf.at[rows(r, FAR[p])], dyf.at[rows(r, FAR[p])], y_send.at[p], y_recv.at[p], rr=over)

    def d_copy(p):
        return send(dyf.at[rows(r, NEAR[p])], dyf.at[rows(r, NEAR[p])], d_send.at[p], d_recv.at[p], rr=mate)

    def e_copy(p):
        return send(dyf.at[rows(over, FAR[p])], dyf.at[rows(over, FAR[p])], e_send.at[p], e_recv.at[p], rr=mate)

    def y_arrival(p):
        return send(dyf.at[rows(over, FAR[p])], dyf.at[rows(over, FAR[p])], y_send.at[p], y_recv.at[p], rr=over)

    def d_arrival(p):
        return send(dyf.at[rows(mate, NEAR[p])], dyf.at[rows(mate, NEAR[p])], d_send.at[p], d_recv.at[p], rr=mate)

    def e_arrival(p):
        at = rows(over_mate, FAR[p])
        return send(dyf.at[at], dyf.at[at], e_send.at[p], e_recv.at[p], rr=mate)

    for p in range(len(NEAR)):
        load(p).wait()
        if p == 0:
            y_copy(0).start()
        d_copy(p).start()

    def y_rest():
        @pl.when(relay)
        def _():
            m_out.wait_recv()
            m_pass.start()

        for p in range(1, len(FAR)):
            y_copy(p).start()

    def x_route(t):
        near = y == t // 2
        head = jnp.where(jnp.logical_or(near, t % 2 == 0), r, (r + 2) % 4)
        hops = jnp.where(z >= head, z - head, head - z)
        turn = jnp.where(near, t % 2, 2 + t % 2)
        go_right = jnp.logical_and(z >= head, z < 3)
        go_left = jnp.logical_and(z <= head, z > 0)
        return turn + hops, go_right, go_left

    routes = [x_route(t) for t in range(4)]

    def x_right_copy(t):
        return send(xf.at[xrows(t)], xf.at[xrows(t)], x_right.at[t], x_recv.at[t], c=z + 1)

    def x_left_copy(t):
        return send(xf.at[xrows(t)], xf.at[xrows(t)], x_left.at[t], x_recv.at[t], c=z - 1)

    def x_point(j):
        for t in range(4):
            when, go_right, go_left = routes[t]
            live = when == j

            @pl.when(live)
            def _():
                pltpu.make_async_copy(x_ref, xf.at[xrows(t)], x_recv.at[t]).wait()

            @pl.when(jnp.logical_and(live, go_right))
            def _():
                x_right_copy(t).start()

            @pl.when(jnp.logical_and(live, go_left))
            def _():
                x_left_copy(t).start()

    def blocks(s):
        return (r, mate, NEAR[s]) if s < len(NEAR) else (over, over_mate, FAR[s - len(NEAR)])

    def size(s):
        return blocks(s)[2][1] * unit

    inner = jnp.logical_or(z == 1, z == 2)
    end = jnp.logical_not(inner)
    far_end = 3 * (1 - zh)

    def at(first, n, count=1):
        return pl.ds(pl.multiple_of(first * n, n), count * n)

    def z1_end(s):
        n = size(s) // 2
        src = pbuf.at[s % SLOTS, at(1 - zh, n, 3)]
        return send(src, rb1.at[s, pl.ds(0, 3 * n)], z1_send.at[s], z1_recv.at[s], c=z1)

    def z1_inner(s):
        n = size(s) // 2
        src = pbuf.at[s % SLOTS, at(3 * zh, n)]
        return send(src, rb1.at[s, pl.ds(0, n)], z1_send.at[s], z1_recv.at[s], c=z1)

    def z2_copy(s):
        n = size(s) // 2
        return send(pbuf.at[s % SLOTS, at(3 - z, n)], rb2.at[s, pl.ds(0, n)], z2_send.at[s], z2_recv.at[s], c=3 - z)

    def z3_copy(s):
        n = size(s) // 2
        src = pbuf.at[s % SLOTS, at(far_end, n)]
        return send(src, rb2.at[s, pl.ds(0, n)], z3_send.at[s], z2_recv.at[s], c=far_end)

    def z_sent(s):
        @pl.when(end)
        def _():
            z1_end(s).wait_send()

        @pl.when(inner)
        def _():
            z1_inner(s).wait_send()
            z2_copy(s).wait_send()
            z3_copy(s).wait_send()

    def f_start(s, begin):
        a, b, span = blocks(s)
        n = size(s) // 2
        owner = a + zh * (b - a)
        src = fbuf.at[s, pl.ds(0, n)]
        dst = dx_ref.at[pl.ds(pl.multiple_of(span[0] * unit + zb * n, n), n)]
        away = jnp.logical_or(z != r, owner != r)

        @pl.when(away)
        def _():
            copy = send(src, dst, f_send.at[s], f_recv.at[0], c=r, rr=owner)
            copy.start() if begin else copy.wait_send()

        if begin:

            @pl.when(jnp.logical_not(away))
            def _():
                pltpu.make_async_copy(src, dst, f_recv.at[0]).start()

    def stage_a(s):
        a, b, span = blocks(s)
        p = s - len(NEAR)
        if p < 0:
            d_arrival(s).wait_recv()
        else:
            y_arrival(p).wait_recv()
            e_copy(p).start()
            e_arrival(p).wait_recv()
        if s == 0:
            w_load.wait()
        if s >= SLOTS:
            z_sent(s - SLOTS)
        slot, n = s % SLOTS, 2 * size(s)
        pbuf[slot, :n] = jnp.zeros((n, kb), jnp.float32)

        @pl.loop(0, nb // kc)
        def _(i):
            cols = pl.ds(pl.multiple_of(i * kc, kc), kc)
            lhs = jnp.concatenate([dyf[rows(a, span), cols], dyf[rows(b, span), cols]], axis=0)
            pbuf[slot, :n] += lax.dot_general(
                lhs, wv[:, cols], (((1,), (1,)), ((), ())), preferred_element_type=jnp.float32
            )

        @pl.when(end)
        def _():
            z1_end(s).start()

        @pl.when(inner)
        def _():
            z1_inner(s).start()

    def stage_b(s):
        n = size(s) // 2

        @pl.when(inner)
        def _():
            z1_end(s).wait_recv()
            pbuf[s % SLOTS, at(2 * (1 - zh), n, 2)] += rb1[s, at(1 - zh, n, 2)]
            z3_copy(s).start()
            z2_copy(s).start()

    def stage_c(s):
        n = size(s) // 2

        @pl.when(end)
        def _():
            z1_inner(s).wait_recv()

        z2_copy(s).wait_recv()
        mine = jnp.where(inner, 2 * zh, 0)
        total = (pbuf[s % SLOTS, at(z, n)] + rb1[s, at(mine, n)]) + rb2[s, :n]
        fbuf[s, :n] = total.astype(fbuf.dtype)
        f_start(s, True)

    def o_copy(j, slot):
        cols = pl.ds(pl.multiple_of(j * nc, nc), nc)
        return pltpu.make_async_copy(obuf.at[slot], dw_ref.at[:, cols], o_sem.at[slot])

    early = [pl.ds(pl.multiple_of(y * 2 * tb, 2 * tb), 2 * tb), rows(2 * (1 - y), (0, LATE)), rows(3 - 2 * y, (0, LATE))]

    def dw_early(lo, hi):
        chunks = nb // nc

        @pl.loop((lo * chunks) // 14, (hi * chunks) // 14)
        def _(j):
            slot = j % 2

            @pl.when(j >= 2)
            def _():
                o_copy(j - 2, slot).wait()

            cols = pl.ds(pl.multiple_of(j * nc, nc), nc)
            terms = [
                lax.dot_general(xf[at], dyf[at, cols], (((0,), (0,)), ((), ())), preferred_element_type=jnp.float32)
                for at in early
            ]
            obuf[slot] = (terms[0] + terms[1]) + terms[2]
            o_copy(j, slot).start()

    late = (8 - LATE) * unit

    def x_late(i):
        src = xf.at[rows((over, over_mate)[i], (LATE, 8 - LATE))]
        return pltpu.make_async_copy(src, xl_ref.at[pl.ds(i * late, late)], l_sem.at[i])

    def dy_late(i):
        src = dyf.at[rows((over, over_mate)[i], (LATE, 8 - LATE))]
        return pltpu.make_async_copy(src, dyl_ref.at[pl.ds(i * late, late)], l_sem.at[2 + i])

    stage_a(0)
    x_point(0)
    stage_a(1)
    y_rest()
    stage_a(2)
    stage_a(3)
    stage_b(0)
    stage_b(1)
    stage_c(0)
    x_point(1)
    stage_b(2)
    stage_c(1)
    stage_a(4)
    stage_b(3)
    stage_c(2)
    x_point(2)
    stage_c(3)
    stage_b(4)
    x_point(3)
    stage_c(4)
    stage_a(5)
    stage_b(5)
    x_point(4)
    stage_c(5)
    stage_a(6)
    x_point(5)
    stage_b(6)
    stage_a(7)
    stage_c(6)
    stage_b(7)
    stage_a(8)
    dy_late(0).start()
    dy_late(1).start()
    x_point(6)
    x_late(0).start()
    x_late(1).start()
    dw_early(0, 5)
    stage_c(7)
    stage_b(8)
    dw_early(5, 10)
    stage_c(8)
    dw_early(10, 14)

    chunks = nb // nc
    for j in (chunks - 2, chunks - 1):
        o_copy(j, j % 2).wait()
    for p in range(len(NEAR)):
        d_copy(p).wait_send()
    for p in range(len(FAR)):
        y_copy(p).wait_send()
        e_copy(p).wait_send()
    for s in range(STEPS - SLOTS, STEPS):
        z_sent(s)
    for s in range(STEPS):
        f_start(s, False)
    for t in range(4):
        _, go_right, go_left = routes[t]

        @pl.when(go_right)
        def _():
            x_right_copy(t).wait_send()

        @pl.when(go_left)
        def _():
            x_left_copy(t).wait_send()

    @pl.when(direct)
    def _():
        x_out.wait_send()

    @pl.when(detour)
    def _():
        m_out.wait_send()

    @pl.when(relay)
    def _():
        m_pass.wait_send()

    for i in range(2):
        x_late(i).wait()
        dy_late(i).wait()
    pltpu.make_async_copy(dx_ref, dx_ref, f_recv.at[0]).wait()


def solution(mesh):
    rows = P(("data", "r"), "c")

    def local(x, w, dy):
        tb, kb = x.shape
        nb = dy.shape[1]
        pr, late = tb // 4, 2 * tb * (8 - LATE) // 8
        nc = pick(nb, 512)
        any_spec = pl.BlockSpec(memory_space=pl.ANY)
        dma = pltpu.SemaphoreType.DMA
        far, steps = (len(FAR),), (STEPS,)
        dx, dw_early, x_late, dy_late = pl.pallas_call(
            kernel,
            name="linear_backward",
            out_shape=(
                jax.ShapeDtypeStruct((tb, kb), jnp.bfloat16),
                jax.ShapeDtypeStruct((kb, nb), jnp.float32),
                jax.ShapeDtypeStruct((late, kb), jnp.bfloat16),
                jax.ShapeDtypeStruct((late, nb), jnp.bfloat16),
            ),
            in_specs=[any_spec] * 3,
            out_specs=(any_spec,) * 4,
            scratch_shapes=[
                pltpu.VMEM((4 * tb, nb), jnp.bfloat16),
                pltpu.VMEM((kb, nb), jnp.bfloat16),
                pltpu.VMEM((4 * tb, kb), jnp.bfloat16),
                pltpu.VMEM((tb, kb), jnp.bfloat16),
                pltpu.VMEM((SLOTS, 2 * pr, kb), jnp.float32),
                pltpu.VMEM((STEPS, 3 * pr // 2, kb), jnp.float32),
                pltpu.VMEM((STEPS, pr // 2, kb), jnp.float32),
                pltpu.VMEM((STEPS, pr // 2, kb), jnp.bfloat16),
                pltpu.VMEM((2, kb, nc), jnp.float32),
                dma((len(NEAR),)), dma, dma(far), dma(far), dma((len(NEAR),)), dma((len(NEAR),)), dma(far), dma(far),
                dma(steps), dma(steps), dma(steps), dma(steps), dma(steps), dma(steps), dma((1,)),
                dma((1,)), dma((4,)), dma((4,)), dma((4,)), dma((3,)), dma((2,)), dma((4,)),
            ],
            compiler_params=pltpu.CompilerParams(
                collective_id=0, has_side_effects=True, vmem_limit_bytes=67_000_000
            ),
        )(x, w, dy)
        dw_late = lax.dot_general(x_late, dy_late, (((0,), (0,)), ((), ())), preferred_element_type=jnp.float32)
        return dx, dw_early + dw_late

    return jax.shard_map(local, mesh=mesh, in_specs=(rows, P("r", "c"), rows), out_specs=(rows, rows), check_vma=False)
```
